128 devices in a mesh: slab: 32 (over y, z, core), md: 4 (over x).
Axes of the slice: x: 4, y: 4, z: 4, core: 2. Of those that a mesh axis runs over, the one named last changes fastest.
Arguments:
- populations: float32 [19, 64, 256, 128], P(None, 'slab', 'md'), may hold values from 0.02 to 0.1
- relax: float32 [64, 256, 128], P('slab', 'md'), may hold values from 0.8 to 1.8
- owners: int32 [64, 256, 2], P('slab', 'md'), may hold values from 0 to 127, all different within a row; in each aligned block of 64 rows (0 to 63, 64 to 127, ..., all dimensions but the last counted through in order) at most 2 rows name the same one
- positions: float32 [3, 131072], P(None, ('slab', 'md')), may hold values from 0 to 3
- velocities: float32 [3, 131072], P(None, ('slab', 'md')), may hold values from -5 to 5
- neighbours: int32 [131072, 64], P(('slab', 'md')), may hold values from 0 to 1023
- atom_slots: int32 [131072], P(('slab', 'md')), may hold values from 0 to 511
Outputs:
- populations_out: float32 [19, 64, 256, 128], P(None, 'slab', 'md')
- positions_out: float32 [3, 131072], P(None, ('slab', 'md'))
- velocities_out: float32 [3, 131072], P(None, ('slab', 'md'))
- cell_moments: float32 [4, 64, 256], P(None, 'slab', 'md')
The draws below stay inside these ranges and needn't reach their ends.
Inputs may be any that keep to these rules, and one draw needn't show every extreme that they name: The 64 entries of one z position on one device name any owner at most 2 times in each column k and across k; the 2 owners of one cell differ. `neighbours`: entries index atoms of the same subdomain's block of 1024 atoms; an atom that lists itself is padding.
All inputs are finite; a program needn't handle non-finite values.
Results may differ from the reference program's by a relative error of at most 0.0003.
Values sent between devices are 32-bit elements; how exact they have to be, the bound alone decides.
No kernel may reach another device: no remote copies, remote signals or barrier semaphores. Data moves between devices by JAX's collectives and lax.ppermute only.
A program may use at most 64 MiB of HBM per device.

```python
import math
import jax
import jax.numpy as jnp
import numpy as np
from jax import lax

CZ = 2
CX = 64
NY = 128
ATOMS = 1024
NBR = 64
TOP = 2
LB_STEPS = 4
MD_STEPS = 5
NZ = 64
NX = 256
ATOMS_ALL = 131072
MOST = 2
CAP = 4
SLOTS = 512
N_SLAB = 32
N_MD = 4
DEVICES = 128


def plant(values, own_key, smallest, top_value):
    longest = values.shape.index(max(values.shape))
    spots = []
    for shift in (0, 1):
        where = [jax.random.randint(jax.random.fold_in(own_key, axis), (), 0, length) for axis, length in enumerate(values.shape)]
        where[longest] = (where[longest] + shift) % values.shape[longest]
        spots.append(tuple(where))
    return values.at[spots[0]].set(smallest).at[spots[1]].set(top_value)


def block_scale(stream_key, shape, cuts, low, high):
    def one(position, shards_of):
        steps = jax.random.uniform(jax.random.fold_in(jax.random.fold_in(stream_key, 6), position), (shards_of,), jnp.float32, low / len(cuts), high / len(cuts))
        return jnp.repeat(jnp.exp(steps), shape[position] // shards_of).reshape((-1,) + (1,) * (len(shape) - position - 1))

    gain = one(*cuts[0])
    for cut in cuts[1:]:
        gain = gain * one(*cut)
    return gain


def deal_out(key, own, number, rows, count, top, bound, lean):
    sequence = jax.random.permutation(key, count)
    packed, common = load_shares(count, rows * top, bound, lean, True), load_shares(count, rows * top, bound, lean, False)
    places = jnp.arange(count)

    def named(lengths, turn):
        used = int((lengths > 0).sum())
        fixed = max(1, used // 4)
        moved = fixed + (places - fixed + turn * (used - fixed)) % max(1, count - fixed)
        return jnp.zeros((count,), jnp.int32).at[sequence[jnp.where(places < fixed, places, moved)]].set(jnp.asarray(lengths, jnp.int32))

    lengths = jnp.where(number % 4 == 0, named(packed, number // 4), named(common, number - number // 4 - 1))
    mixed = jax.random.permutation(jax.random.fold_in(own, 3), count)
    giver, taker = mixed[0:count // 2 * 2:2], mixed[1:count // 2 * 2:2]
    slack = jnp.minimum(lengths[giver] - 1, bound - lengths[taker]) // 2
    slack = jnp.where((giver == sequence[0]) | (taker == sequence[0]) | (lengths[taker] == 0), 0, jnp.maximum(slack, 0))
    moved = jax.random.randint(jax.random.fold_in(own, 4), (count // 2,), 0, 1 << 20) % (slack + 1)
    lengths = lengths.at[giver].add(-moved).at[taker].add(moved)
    items = jnp.searchsorted(jnp.cumsum(lengths), jnp.arange(rows * top), side="right").astype(jnp.int32)
    listing = items.reshape(top, rows).T
    listing = listing[jax.random.permutation(jax.random.fold_in(own, 1), rows)]
    turn = jax.random.randint(jax.random.fold_in(own, 2), (rows, 1), 0, top)
    return jnp.take_along_axis(listing, (jnp.arange(top)[None, :] + turn) % top, axis=1)


def load_shares(amount, total, reach, skew, full):
    loads = [(1 << 20) // math.isqrt(grade ** skew) + 1 for grade in range(1, amount + 1)]
    largest = reach if full else min(reach, max(-(-total // amount), total * loads[0] // sum(loads)))
    least = 1 if total - largest >= amount - 1 else 0
    counts, spare = [largest] + [least] * (amount - 1), total - largest - least * (amount - 1)
    while spare > 0:
        movable = [i for i in range(1, amount) if counts[i] < largest] or [i for i in range(1, amount) if counts[i] < reach]
        whole, budget = sum([loads[i] for i in movable]), spare
        for i in movable:
            more = min(reach - counts[i], max(1, budget * loads[i] // whole), spare)
            counts[i] = counts[i] + more
            spare = spare - more
    return np.array(counts)


def bell_draw(rng, dims, deviation, limit, cuts=(), kind=jnp.bfloat16):
    drawn = deviation * jax.random.normal(rng, dims, jnp.float32)
    if cuts:
        drawn = drawn * block_scale(rng, dims, cuts, -0.22, 0.18)
    return jnp.clip(drawn, -limit, limit).astype(kind)


def setup_inputs(seed: int = 0) -> dict:
    keys = jax.random.split(jax.random.key(seed), 8)
    populations = jnp.clip(0.02 + 0.08 * jax.random.uniform(keys[0], (19, NZ, NX, NY), jnp.float32) ** block_scale(keys[0], (19, NZ, NX, NY), ((1, 32), (2, 4)), -0.2, 0.2), 0.02, 0.1)
    relax = jnp.clip(jnp.exp(math.log(1.8) - 0.8109302 * jax.random.uniform(keys[1], (NZ, NX, NY), jnp.float32) ** block_scale(keys[1], (NZ, NX, NY), ((0, 32), (1, 4)), -0.2, 0.2)), 0.8, 1.8)
    owners_keys = jax.random.split(jax.random.fold_in(keys[2], 1), NZ * NX // CX)
    owners_turns = jax.random.permutation(jax.random.fold_in(keys[2], 3), NZ * NX // CX)
    owners = jax.vmap(lambda own, number: deal_out(jax.random.fold_in(keys[2], 2), own, number, CX, DEVICES, TOP, MOST, 2))(owners_keys, owners_turns).reshape((NZ, NX, TOP))
    positions = jnp.clip(3.0 * jax.random.uniform(keys[3], (3, ATOMS_ALL), jnp.float32) ** block_scale(keys[3], (3, ATOMS_ALL), ((1, 128),), -0.2, 0.2), 0.0, 3.0)
    velocities = bell_draw(keys[4], (3, ATOMS_ALL), 1.0, 5.0, ((1, 128),), jnp.float32)
    neighbours = plant(jax.random.randint(keys[5], (ATOMS_ALL, NBR), 0, ATOMS), jax.random.fold_in(keys[5], 1), 0, ATOMS - 1).astype(jnp.int32)
    atom_slots = plant(jax.random.randint(keys[6], (ATOMS_ALL,), 0, SLOTS), jax.random.fold_in(keys[6], 1), 0, SLOTS - 1).astype(jnp.int32)
    return dict(populations=populations, relax=relax, owners=owners, positions=positions, velocities=velocities, neighbours=neighbours, atom_slots=atom_slots)


lattice_dirs = [(0, 0, 0), (1, 0, 0), (-1, 0, 0), (0, 1, 0), (0, -1, 0), (0, 0, 1), (0, 0, -1),
                (1, 1, 0), (-1, -1, 0), (1, -1, 0), (-1, 1, 0), (1, 0, 1), (-1, 0, -1), (1, 0, -1),
                (-1, 0, 1), (0, 1, 1), (0, -1, -1), (0, 1, -1), (0, -1, 1)]
lattice_weights = [1.0 / 3.0] + [1.0 / 18.0] * 6 + [1.0 / 36.0] * 12
velocity_scale = 10.0
pair_strength = 0.5
friction = 2.0
time_step = 0.1


def velocity(f, density):
    comps = []
    for axis_id in range(3):
        total = jnp.zeros_like(density)
        for index, direction in enumerate(lattice_dirs):
            if direction[axis_id] != 0:
                total = total + direction[axis_id] * f[index]
        comps.append(total / density)
    return comps


def collide(f, relax):
    density = jnp.sum(f, axis=0)
    vel_x, vel_y, vel_z = velocity(f, density)
    usq = vel_x * vel_x + vel_y * vel_y + vel_z * vel_z
    result = []
    for index, direction in enumerate(lattice_dirs):
        along = direction[0] * vel_x + direction[1] * vel_y + direction[2] * vel_z
        equil = lattice_weights[index] * density * (1.0 + 3.0 * along + 4.5 * along * along - 1.5 * usq)
        result.append(f[index] - relax * (f[index] - equil))
    return result


def md_run(pos, vel, nbr, slots, recv):
    target = recv[slots]
    goal = target[:, :3].T
    dens = target[:, 3]
    for step in range(MD_STEPS):
        gap = pos[:, nbr] - pos[:, :, None]
        weight = jnp.exp(-0.5 * jnp.sum(gap * gap, axis=0))
        force = pair_strength * jnp.sum(gap * weight[None], axis=2) + friction * dens[None, :] * (goal - vel)
        vel = vel + time_step * force
        pos = pos + time_step * vel
    data = jnp.concatenate([vel, jnp.sum(vel * vel, axis=0, keepdims=True)], axis=0).T
    sums = jax.ops.segment_sum(data, slots, num_segments=recv.shape[0])
    count = jax.ops.segment_sum(jnp.ones(slots.shape, jnp.float32), slots, num_segments=recv.shape[0])
    return pos, vel, sums / jnp.maximum(count, 1.0)[:, None]


def reference(populations, relax, owners, positions, velocities, neighbours, atom_slots):
    f = populations
    for step in range(LB_STEPS):
        post = collide(f, relax)
        f = jnp.stack([jnp.roll(post[i], (c[2], c[0], c[1]), axis=(0, 1, 2)) for i, c in enumerate(lattice_dirs)])
    density = jnp.sum(f, axis=0)
    vel_x, vel_y, vel_z = velocity(f, density)
    targets = jnp.stack([jnp.mean(velocity_scale * vel_x, axis=2), jnp.mean(velocity_scale * vel_y, axis=2),
                         jnp.mean(velocity_scale * vel_z, axis=2), jnp.mean(density, axis=2)])
    devices = N_SLAB * N_MD
    entries = CZ * CX * TOP
    tgt_dev = targets.reshape(4, N_SLAB, CZ, N_MD, CX).transpose(1, 3, 0, 2, 4).reshape(devices, 4, CZ * CX)
    vals = jnp.repeat(tgt_dev, TOP, axis=2).transpose(0, 2, 1)
    own = owners.reshape(N_SLAB, CZ, N_MD, CX, TOP).transpose(0, 2, 1, 3, 4).reshape(devices, entries)
    labels = jnp.arange(devices, dtype=jnp.int32)

    def ranks_of(row):
        onehot = (row[:, None] == labels[None, :]).astype(jnp.int32)
        before = jnp.cumsum(onehot, axis=0) - onehot
        return jnp.sum(before * onehot, axis=1).astype(jnp.int32)

    rank = lax.map(ranks_of, own)
    slot = (labels[:, None] * CAP + rank).astype(jnp.int32)
    pos_dev = positions.reshape(3, devices, ATOMS).transpose(1, 0, 2)
    vel_dev = velocities.reshape(3, devices, ATOMS).transpose(1, 0, 2)
    nbr_dev = neighbours.reshape(devices, ATOMS, NBR)
    slot_dev = atom_slots.reshape(devices, ATOMS)

    def per_owner(back, inputs):
        owner_id, pos, vel, nbr, slots = inputs
        hit = own == owner_id
        where_to = jnp.where(hit, slot, SLOTS).astype(jnp.int32)
        recv = jnp.zeros((SLOTS, 4), jnp.float32).at[where_to].set(vals, mode="drop")
        pos, vel, moms = md_run(pos, vel, nbr, slots, recv)
        back = back + jnp.where(hit[:, :, None], moms[slot], 0.0)
        return back, (pos, vel)

    back, (pos_out, vel_out) = lax.scan(per_owner, jnp.zeros((devices, entries, 4), jnp.float32),
                                        (labels, pos_dev, vel_dev, nbr_dev, slot_dev))
    summed = back.reshape(devices, CZ * CX, TOP, 4).sum(axis=2).transpose(0, 2, 1)
    cell_moments = summed.reshape(N_SLAB, N_MD, 4, CZ, CX).transpose(2, 0, 3, 1, 4).reshape(4, NZ, NX)
    positions_out = pos_out.transpose(1, 0, 2).reshape(3, ATOMS_ALL)
    velocities_out = vel_out.transpose(1, 0, 2).reshape(3, ATOMS_ALL)
    return f, positions_out, velocities_out, cell_moments
```

```python
import jax
import jax.numpy as jnp
from jax import lax
from jax.experimental import pallas as pl
from jax.experimental.pallas import tpu as pltpu
from jax.sharding import PartitionSpec as P

LB_STEPS = 4
MD_STEPS = 5
f32 = jnp.float32
i32 = jnp.int32
bf16 = jnp.bfloat16

lattice_dirs = [
    (0, 0, 0),
    (1, 0, 0),
    (-1, 0, 0),
    (0, 1, 0),
    (0, -1, 0),
    (0, 0, 1),
    (0, 0, -1),
    (1, 1, 0),
    (-1, -1, 0),
    (1, -1, 0),
    (-1, 1, 0),
    (1, 0, 1),
    (-1, 0, -1),
    (1, 0, -1),
    (-1, 0, 1),
    (0, 1, 1),
    (0, -1, -1),
    (0, 1, -1),
    (0, -1, 1),
]
lattice_weights = [1.0 / 3.0] + [1.0 / 18.0] * 6 + [1.0 / 36.0] * 12
velocity_scale = 10.0
pair_strength = 0.5
friction = 2.0
time_step = 0.1


def padded_2(cells, sides, width):
    for axis, dim in sides:
        count = lax.axis_size(axis)
        head = lax.slice_in_dim(cells, 0, width, axis=dim)
        tail = lax.slice_in_dim(cells, cells.shape[dim] - width, cells.shape[dim], axis=dim)
        cells = jnp.concatenate(
            [
                lax.ppermute(tail, axis, [(i, (i + 1) % count) for i in range(count)]),
                cells,
                lax.ppermute(head, axis, [((i + 1) % count, i) for i in range(count)]),
            ],
            axis=dim,
        )
    return cells


def shifted(shard, axis, by):
    devices = lax.axis_size(axis)
    return lax.ppermute(shard, axis, [(i, (i + by) % devices) for i in range(devices)])


def velocity(f, density):
    comps = []
    for axis_id in range(3):
        total = jnp.zeros_like(density)
        for index, direction in enumerate(lattice_dirs):
            if direction[axis_id] != 0:
                total = total + direction[axis_id] * f[index]
        comps.append(total / density)
    return comps


def collide(f, relax):
    density = jnp.sum(f, axis=0)
    vel_x, vel_y, vel_z = velocity(f, density)
    usq = vel_x * vel_x + vel_y * vel_y + vel_z * vel_z
    result = []
    for index, direction in enumerate(lattice_dirs):
        along = direction[0] * vel_x + direction[1] * vel_y + direction[2] * vel_z
        equil = (
            lattice_weights[index] * density * (1.0 + 3.0 * along + 4.5 * along * along - 1.5 * usq)
        )
        result.append(f[index] - relax * (f[index] - equil))
    return result


def lanes(table, index):
    return jnp.take_along_axis(table, index, axis=1, mode="promise_in_bounds")


def spread(block, index, rows=8):
    return jnp.broadcast_to(block[index : index + 1, :], (rows, 128))


def pair_sum(coords, nbr_ref):
    tables = [[spread(comp, chunk) for chunk in range(8)] for comp in coords]

    def entry(k, total):
        index = nbr_ref[k]
        low = index & 127
        bits = [(index & mask) != 0 for mask in (128, 256, 512)]
        gaps = []
        for comp in range(3):
            level = [lanes(table, low) for table in tables[comp]]
            for bit in bits:
                level = [
                    jnp.where(bit, level[2 * j + 1], level[2 * j]) for j in range(len(level) // 2)
                ]
            gaps.append(level[0] - coords[comp])
        weight = jnp.exp(-0.5 * (gaps[0] * gaps[0] + gaps[1] * gaps[1] + gaps[2] * gaps[2]))
        return tuple(t + g * weight for t, g in zip(total, gaps))

    zero = jnp.zeros((8, 128), f32)
    return lax.fori_loop(0, nbr_ref.shape[0], entry, (zero, zero, zero), unroll=16)


def prep_kernel(own_ref, slot_ref, pos_ref, vel_ref, nbr_ref,
                inv_ref, rank_ref, hot_ref, icnt_ref, force_ref, p8_ref, v8_ref):
    row_id = lax.broadcasted_iota(i32, (128, 128), 0)
    lane_id = lax.broadcasted_iota(i32, (128, 128), 1)
    own = [spread(own_ref[...], k, 128) for k in range(2)]
    own_t = [o.T for o in own]
    ranks = []
    for k in range(2):
        count = jnp.zeros((128, 128), i32)
        for other in range(2):
            count = count + jnp.where((own_t[other] == own[k]) & (row_id < lane_id), 1, 0)
        ranks.append(jnp.sum(count, axis=0, keepdims=True))
    rank_ref[...] = jnp.concatenate(ranks + [jnp.zeros((6, 128), i32)], axis=0)
    rank_t = [jnp.broadcast_to(r, (128, 128)).T for r in ranks]
    rows = []
    for r in range(4):
        cell = jnp.zeros((128, 128), i32)
        for k in range(2):
            cell = cell + jnp.where((own_t[k] == lane_id) & (rank_t[k] == r), row_id + 1, 0)
        rows.append(jnp.sum(cell, axis=0, keepdims=True) - 1)
    inv_ref[...] = jnp.concatenate(rows + [jnp.zeros((4, 128), i32)], axis=0)
    slots = slot_ref[...]
    count = jnp.zeros((128, 16), f32)
    want = lax.broadcasted_iota(i32, (16, 128), 0) >> 2
    for s in range(8):
        one = spread(slots, s, 128)
        hot = jnp.where((one >> 2) == row_id, 1.0, 0.0).astype(bf16)
        hot_ref[:, s * 128 : (s + 1) * 128] = hot
        match = jnp.where((spread(slots, s, 16) & 3) == want, 1.0, 0.0).astype(bf16)
        count = count + lax.dot_general(
            hot, match, (((1,), (1,)), ((), ())), preferred_element_type=f32
        )
    icnt_ref[...] = 1.0 / jnp.maximum(count, 1.0)
    for c in range(3):
        for s in range(8):
            p8_ref[c, s : s + 1, :] = pos_ref[c : c + 1, s * 128 : (s + 1) * 128]
            v8_ref[c, s : s + 1, :] = vel_ref[c : c + 1, s * 128 : (s + 1) * 128]
    total = pair_sum([p8_ref[0], p8_ref[1], p8_ref[2]], nbr_ref)
    for c in range(3):
        force_ref[c] = total[c]


def pack_kernel(t_ref, inv_ref, out_ref):
    t16 = jnp.concatenate([t_ref[...]] * 4, axis=0)
    inv16 = jnp.concatenate(
        [jnp.broadcast_to(inv_ref[r : r + 1, :], (4, 128)) for r in range(4)], axis=0
    )
    picked = jnp.where(inv16 >= 0, lanes(t16, jnp.maximum(inv16, 0)), 0.0)
    out_ref[...] = jnp.concatenate([picked, jnp.zeros((112, 128), f32)], axis=0).T


def md_kernel(arr_ref, p8_ref, v8_ref, force_ref, nbr_ref, slot_ref, hot_ref, icnt_ref,
              pos_ref, vel_ref, mom_ref):
    table = arr_ref[...].T
    slots = slot_ref[...]
    source = slots >> 2
    which = slots & 3
    target = []
    for c in range(4):
        value = lanes(spread(table, c), source)
        for r in range(1, 4):
            value = jnp.where(which == r, lanes(spread(table, r * 4 + c), source), value)
        target.append(value)
    drag = friction * target[3]
    pos = [p8_ref[c] for c in range(3)]
    vel = [v8_ref[c] for c in range(3)]
    for step in range(MD_STEPS):
        pair = [force_ref[c] for c in range(3)] if step == 0 else pair_sum(pos, nbr_ref)
        for c in range(3):
            force = pair_strength * pair[c] + drag * (target[c] - vel[c])
            vel[c] = vel[c] + time_step * force
            pos[c] = pos[c] + time_step * vel[c]
    speed = vel[0] * vel[0] + vel[1] * vel[1] + vel[2] * vel[2]
    data = vel + [speed]
    row_id = lax.broadcasted_iota(i32, (16, 128), 0)
    comp = row_id & 3
    sums = jnp.zeros((128, 16), f32)
    for s in range(8):
        value = spread(data[0], s, 16)
        for c in range(1, 4):
            value = jnp.where(comp == c, spread(data[c], s, 16), value)
        value = jnp.where((spread(slots, s, 16) & 3) == (row_id >> 2), value, 0.0)
        hot = hot_ref[:, s * 128 : (s + 1) * 128]
        for part in range(3):
            piece = value.astype(bf16)
            value = value - piece.astype(f32)
            sums = sums + lax.dot_general(
                hot, piece, (((1,), (1,)), ((), ())), preferred_element_type=f32
            )
    mom_ref[...] = jnp.zeros((128, 128), f32)
    mom_ref[:, :16] = sums * icnt_ref[...]
    for c in range(3):
        for s in range(8):
            pos_ref[c : c + 1, s * 128 : (s + 1) * 128] = pos[c][s : s + 1, :]
            vel_ref[c : c + 1, s * 128 : (s + 1) * 128] = vel[c][s : s + 1, :]


def cell_kernel(back_ref, own_ref, rank_ref, out_ref):
    table = back_ref[...].T[:16, :]
    which = lax.broadcasted_iota(i32, (16, 128), 0) >> 2
    total = jnp.zeros((16, 128), f32)
    for k in range(2):
        picked = lanes(table, spread(own_ref[...], k, 16))
        total = total + jnp.where(spread(rank_ref[...], k, 16) == which, picked, 0.0)
    cell = total[0:4] + total[4:8] + total[8:12] + total[12:16]
    out_ref[:, 0, :] = cell[:, :64]
    out_ref[:, 1, :] = cell[:, 64:]


def shape(*dims, dtype=f32):
    return jax.ShapeDtypeStruct(dims, dtype)


def exchange(rows):
    return lax.all_to_all(rows, ("slab", "md"), split_axis=0, concat_axis=0, tiled=True)


def on_device(populations, relax, owners, positions, velocities, neighbours, atom_slots):
    own = owners.reshape(128, 2).T
    slots = atom_slots.reshape(8, 128)
    nbr = neighbours.reshape(8, 128, 64).transpose(2, 0, 1)
    inv, rank, hot, icnt, force, p8, v8 = pl.pallas_call(
        prep_kernel,
        out_shape=(
            shape(8, 128, dtype=i32),
            shape(8, 128, dtype=i32),
            shape(128, 1024, dtype=bf16),
            shape(128, 16),
            shape(3, 8, 128),
            shape(3, 8, 128),
            shape(3, 8, 128),
        ),
        name="prep",
    )(own, slots, positions, velocities, nbr)
    f = populations
    cz_len = f.shape[1]
    cx_len = f.shape[2]
    rising = [i for i, c in enumerate(lattice_dirs) if c[2] == 1]
    falling = [i for i, c in enumerate(lattice_dirs) if c[2] == -1]
    for step in range(LB_STEPS):
        post = jnp.stack(collide(f, relax))
        padded = padded_2(post, (("md", 2),), 1)
        moved = jnp.stack(
            [
                jnp.roll(padded[i, :, 1 - c[0] : 1 - c[0] + cx_len, :], c[1], axis=2)
                for i, c in enumerate(lattice_dirs)
            ]
        )
        top_planes = jnp.stack([moved[i, cz_len - 1 :] for i in rising])
        low_planes = jnp.stack([moved[i, :1] for i in falling])
        below = shifted(top_planes, "slab", 1)
        above = shifted(low_planes, "slab", -1)
        pieces = []
        for i, c in enumerate(lattice_dirs):
            if c[2] == 1:
                pieces.append(
                    jnp.concatenate([below[rising.index(i)], moved[i, : cz_len - 1]], axis=0)
                )
            elif c[2] == -1:
                pieces.append(jnp.concatenate([moved[i, 1:], above[falling.index(i)]], axis=0))
            else:
                pieces.append(moved[i])
        f = jnp.stack(pieces)
    density = jnp.sum(f, axis=0)
    vel_x, vel_y, vel_z = velocity(f, density)
    targets = jnp.stack(
        [
            jnp.mean(velocity_scale * vel_x, axis=2),
            jnp.mean(velocity_scale * vel_y, axis=2),
            jnp.mean(velocity_scale * vel_z, axis=2),
            jnp.mean(density, axis=2),
        ]
    )
    outgoing = pl.pallas_call(pack_kernel, out_shape=shape(128, 128), name="pack")(
        targets.reshape(4, 128), inv
    )
    arrived = exchange(outgoing)
    pos_out, vel_out, moms = pl.pallas_call(
        md_kernel, out_shape=(shape(3, 1024), shape(3, 1024), shape(128, 128)), name="md"
    )(arrived, p8, v8, force, nbr, slots, hot, icnt)
    returned = exchange(moms)
    cell = pl.pallas_call(cell_kernel, out_shape=shape(4, 2, 64), name="cells")(
        returned, own, rank
    )
    return (f, pos_out, vel_out, cell)


def solution(mesh):
    return jax.shard_map(
        on_device,
        mesh=mesh,
        in_specs=(
            P(None, "slab", "md", None),
            P("slab", "md", None),
            P("slab", "md", None),
            P(None, ("slab", "md")),
            P(None, ("slab", "md")),
            P(("slab", "md"), None),
            P(("slab", "md")),
        ),
        out_specs=(
            P(None, "slab", "md", None),
            P(None, ("slab", "md")),
            P(None, ("slab", "md")),
            P(None, "slab", "md"),
        ),
        check_vma=False,
    )
```

```python
import jax
import jax.numpy as jnp
from jax import lax
from jax.experimental import pallas as pl
from jax.experimental.pallas import tpu as pltpu
from jax.sharding import PartitionSpec as P

MD_STEPS = 5
f32 = jnp.float32
i32 = jnp.int32
bf16 = jnp.bfloat16

lattice_dirs = [
    (0, 0, 0),
    (1, 0, 0),
    (-1, 0, 0),
    (0, 1, 0),
    (0, -1, 0),
    (0, 0, 1),
    (0, 0, -1),
    (1, 1, 0),
    (-1, -1, 0),
    (1, -1, 0),
    (-1, 1, 0),
    (1, 0, 1),
    (-1, 0, -1),
    (1, 0, -1),
    (-1, 0, 1),
    (0, 1, 1),
    (0, -1, -1),
    (0, 1, -1),
    (0, -1, 1),
]
lattice_weights = [1.0 / 3.0] + [1.0 / 18.0] * 6 + [1.0 / 36.0] * 12
velocity_scale = 10.0
pair_strength = 0.5
friction = 2.0
time_step = 0.1


def mirrored(direction):
    return lattice_dirs.index((direction[0], direction[1], -direction[2]))


flip = [mirrored(c) for c in lattice_dirs]
rising = [i for i, c in enumerate(lattice_dirs) if c[2] == 1]
falling = [flip[i] for i in rising]
level = [i for i, c in enumerate(lattice_dirs) if c[2] == 0]
pairs = [(1, 2), (3, 4), (5, 6)] + [(i, i + 1) for i in range(7, 19, 2)]
NEAR = 14
RELAX = 19
ROWS = 72
PAD = 88


def parity():
    return lax.axis_index("slab") & 1


def actual(index, odd):
    return jnp.where(odd == 1, flip[index], index)


def moments_of(f):
    s = {}
    for plus, minus in pairs:
        s[plus] = (f[plus] + f[minus], f[plus] - f[minus])
    density = f[0]
    for plus, _ in pairs:
        density = density + s[plus][0]
    flow = []
    for axis_id in range(3):
        total = None
        for plus, _ in pairs:
            sign = lattice_dirs[plus][axis_id]
            if sign == 0:
                continue
            term = s[plus][1]
            if total is None:
                total = term
            else:
                total = total + term if sign > 0 else total - term
        flow.append(total)
    return density, flow


def collided(f, relax, wanted):
    density, flow = moments_of(f)
    inverse = 1.0 / density
    vel = [j * inverse for j in flow]
    usq = vel[0] * vel[0] + vel[1] * vel[1] + vel[2] * vel[2]
    keep = 1.0 - relax
    gain = relax * density
    base = gain - (1.5 * gain) * usq
    result = {}
    if 0 in wanted:
        result[0] = keep * f[0] + lattice_weights[0] * base
    for plus, minus in pairs:
        if plus not in wanted and minus not in wanted:
            continue
        along = None
        for axis_id in range(3):
            sign = lattice_dirs[plus][axis_id]
            if sign != 0:
                part = vel[axis_id]
                if along is None:
                    along = part
                else:
                    along = along + part if sign > 0 else along - part
        weight = lattice_weights[plus]
        slope = (3.0 * weight) * (gain * along)
        even = weight * base + 1.5 * (along * slope)
        if plus in wanted:
            result[plus] = keep * f[plus] + (even + slope)
        if minus in wanted:
            result[minus] = keep * f[minus] + (even - slope)
    return {i: rolled(v, lattice_dirs[i][1]) for i, v in result.items()}


def rolled(block, by):
    return block if by == 0 else pltpu.roll(block, by % 128, 1)


def put(ref, where, block_id, value):
    ref[(*where, pl.ds(8 + 8 * block_id, 8), slice(None))] = value
    if block_id == 0:
        ref[(*where, pl.ds(8 + ROWS, 1), slice(None))] = value[0:1, :]
    if block_id == 8:
        ref[(*where, pl.ds(7, 1), slice(None))] = value[7:8, :]


def get(ref, where, block_id, shift):
    return ref[(*where, pl.ds(8 + 8 * block_id - shift, 8), slice(None))]


def rows_of(block_id):
    return pl.ds(8 * block_id, 8)


def send_planes(up_ref, down_ref, plane, block, post, relax):
    for k in range(5):
        up_ref[k if plane == 1 else NEAR + k, block, :] = post[rising[k]]
        down_ref[k if plane == 0 else NEAR + k, block, :] = post[falling[k]]
    near_ref = up_ref if plane == 1 else down_ref
    for k, i in enumerate(level):
        near_ref[5 + k, block, :] = post[i]
    if relax is not None:
        near_ref[RELAX, block, :] = relax


everything = set(range(19))


def first_kernel(f_ref, relax_ref, post_ref, up_ref, down_ref, low_ref, high_ref):
    odd = parity()
    for plane in range(2):
        actual_plane = jnp.where(odd == 1, 1 - plane, plane)
        for b in range(8):
            f = {i: f_ref[actual(i, odd), actual_plane, rows_of(b), :] for i in range(19)}
            relax = relax_ref[actual_plane, rows_of(b), :]
            if b in (0, 7):
                edge_ref = low_ref if b == 0 else high_ref
                for i in range(19):
                    edge_ref[i, plane] = f[i]
                edge_ref[RELAX, plane] = relax
            post = collided(f, relax, everything)
            for i in range(19):
                post_ref[i, plane, rows_of(b), :] = post[i]
            send_planes(up_ref, down_ref, plane, rows_of(b), post, relax)


def edge_kernel(low_ref, high_ref, post_ref, up_ref, down_ref, relax_ref):
    head = lax.broadcasted_iota(i32, (8, 128), 0) < 4
    for plane in range(2):
        mixed = [jnp.where(head, high_ref[i, plane], low_ref[i, plane]) for i in range(20)]
        post = collided(dict(enumerate(mixed[:19])), mixed[RELAX], everything)
        relax_ref[plane] = mixed[RELAX]
        for i in range(19):
            post_ref[i, plane] = post[i]
        send_planes(up_ref, down_ref, plane, rows_of(0), post, mixed[RELAX])


def two_steps(own, below, above, relax, second_ref, from_below_ref, from_above_ref):
    for b in range(9):
        for plane in (-1, 0, 1, 2):
            f = {}
            for i, c in enumerate(lattice_dirs):
                source = plane - c[2]
                if source in (0, 1):
                    f[i] = own(i, source, b, c[0])
                else:
                    side = below if source < 0 else above
                    if c[2] == 0:
                        j = 5 + level.index(i)
                    else:
                        j = (rising if c[2] == 1 else falling).index(i)
                        if source in (-2, 3):
                            j = NEAR + j
                    f[i] = side(j, b, c[0])
            wanted = everything
            if plane == -1:
                wanted = set(rising)
            elif plane == 2:
                wanted = set(falling)
            post = collided(f, relax(plane, b), wanted)
            for i, value in post.items():
                if plane == -1:
                    put(from_below_ref, (rising.index(i),), b, value)
                elif plane == 2:
                    put(from_above_ref, (falling.index(i),), b, value)
                else:
                    put(second_ref, (i, plane), b, value)


def streamed(second_ref, from_below_ref, from_above_ref, plane, b):
    f = {}
    for i, c in enumerate(lattice_dirs):
        source = plane - c[2]
        if source == -1:
            f[i] = get(from_below_ref, (rising.index(i),), b, c[0])
        elif source == 2:
            f[i] = get(from_above_ref, (falling.index(i),), b, c[0])
        else:
            f[i] = get(second_ref, (i, source), b, c[0])
    return f


sliding = [k for k, i in enumerate(rising + level + rising) if lattice_dirs[i][0] != 0]
moving = [i for i, c in enumerate(lattice_dirs) if c[0] != 0]


def seamed(seam_ref, slots, at):
    for slot, key in enumerate(slots):
        for part, b in enumerate((7, 8, 0)):
            seam_ref[slot, 8 * part : 8 * part + 8, :] = at(key, b)

    def read(key, b, shift, main):
        if shift == 0:
            return at(key, b)
        slot = slots.index(key)
        if b == 8:
            return seam_ref[slot, 8 - shift : 16 - shift, :]
        if b == 0 and shift == 1:
            return seam_ref[slot, 15:23, :]
        if b == 7 and shift == -1:
            return seam_ref[slot, 1:9, :]
        return main(8 * b - shift)

    return read


def reader(seam_ref, main_ref, edge_ref):
    def at(j, b):
        if edge_ref is None or b < 8:
            return main_ref[j, rows_of(b), :]
        return edge_ref[j, rows_of(0), :]

    read = seamed(seam_ref, sliding, at)
    return lambda j, b, shift: read(j, b, shift, lambda row: main_ref[j, row : row + 8, :])


def own_reader(seam_ref, main_ref, edge_ref):
    def at(key, b):
        i, plane = key
        return main_ref[i, plane, rows_of(b), :] if b < 8 else edge_ref[i, plane]

    read = seamed(seam_ref, [(i, plane) for i in moving for plane in range(2)], at)
    return lambda i, plane, b, shift: read(
        (i, plane), b, shift, lambda row: main_ref[i, plane, row : row + 8, :]
    )


def middle_kernel(post_ref, post_edge_ref, below_ref, above_ref, below_edge_ref, above_edge_ref,
                  relax_ref, relax_edge_ref,
                  third_ref, up_ref, down_ref, relax_out_ref,
                  second_ref, from_below_ref, from_above_ref, below_seam_ref, above_seam_ref,
                  own_seam_ref):
    odd = parity()
    own = own_reader(own_seam_ref, post_ref, post_edge_ref)
    below = reader(below_seam_ref, below_ref, below_edge_ref)
    above = reader(above_seam_ref, above_ref, above_edge_ref)
    for b in range(8):
        relax_out_ref[0, rows_of(b), :] = below_ref[RELAX, rows_of(b), :]
        relax_out_ref[3, rows_of(b), :] = above_ref[RELAX, rows_of(b), :]
        for plane in range(2):
            relax_out_ref[1 + plane, rows_of(b), :] = relax_ref[
                jnp.where(odd == 1, 1 - plane, plane), rows_of(b), :
            ]
    relax_out_ref[0, rows_of(8), :] = below_edge_ref[RELAX, rows_of(0), :]
    relax_out_ref[3, rows_of(8), :] = above_edge_ref[RELAX, rows_of(0), :]
    for plane in range(2):
        relax_out_ref[1 + plane, rows_of(8), :] = relax_edge_ref[plane]

    def relax(plane, b):
        return relax_out_ref[1 + plane, rows_of(b), :]

    two_steps(own, below, above, relax, second_ref, from_below_ref, from_above_ref)
    for b in range(9):
        for plane in range(2):
            f = streamed(second_ref, from_below_ref, from_above_ref, plane, b)
            post = collided(f, relax(plane, b), everything)
            for i in range(19):
                put(third_ref, (i, plane), b, post[i])
            send_planes(up_ref, down_ref, plane, rows_of(b), post, None)


def last_kernel(post_ref, below_ref, above_ref, relax_ref, inv_ref,
                f_ref, out_ref,
                second_ref, from_below_ref, from_above_ref, below_seam_ref, above_seam_ref,
                flow_ref):
    odd = parity()
    below = reader(below_seam_ref, below_ref, None)
    above = reader(above_seam_ref, above_ref, None)

    def own(i, plane, b, shift):
        return get(post_ref, (i, plane), b, shift)

    def relax(plane, b):
        return relax_ref[1 + plane, rows_of(b), :]

    two_steps(own, below, above, relax, second_ref, from_below_ref, from_above_ref)
    upward = jnp.where(odd == 1, -velocity_scale / 128.0, velocity_scale / 128.0)
    for plane in range(2):
        actual_plane = jnp.where(odd == 1, 1 - plane, plane)
        for b in range(8):
            f = streamed(second_ref, from_below_ref, from_above_ref, plane, b)
            for i in range(19):
                f_ref[actual(i, odd), actual_plane, rows_of(b), :] = f[i]
            density, flow = moments_of(f)
            inverse = 1.0 / density
            where = pl.ds(pl.multiple_of(actual_plane * 64 + 8 * b, 8), 8)
            flow_ref[0, where, :] = flow[0] * inverse * (velocity_scale / 128.0)
            flow_ref[1, where, :] = flow[1] * inverse * (velocity_scale / 128.0)
            flow_ref[2, where, :] = flow[2] * inverse * upward
            flow_ref[3, where, :] = density * (1.0 / 128.0)
    means = [jnp.sum(flow_ref[c].T, axis=0, keepdims=True) for c in range(4)]
    packed = jnp.concatenate(means * 4, axis=0)
    inv16 = jnp.concatenate(
        [jnp.broadcast_to(inv_ref[r : r + 1, :], (4, 128)) for r in range(4)], axis=0
    )
    picked = jnp.where(inv16 >= 0, lanes(packed, jnp.maximum(inv16, 0)), 0.0)
    out_ref[...] = jnp.concatenate([picked, jnp.zeros((112, 128), f32)], axis=0).T


def lanes(table, index):
    return jnp.take_along_axis(table, index, axis=1, mode="promise_in_bounds")


def spread(block, index, rows=8):
    return jnp.broadcast_to(block[index : index + 1, :], (rows, 128))


def pair_sum(coords, nbr_ref):
    tables = [[spread(comp, chunk) for chunk in range(8)] for comp in coords]

    def entry(k, total):
        index = nbr_ref[k]
        low = index & 127
        bits = [(index & mask) != 0 for mask in (128, 256, 512)]
        gaps = []
        for comp in range(3):
            level = [lanes(table, low) for table in tables[comp]]
            for bit in bits:
                level = [
                    jnp.where(bit, level[2 * j + 1], level[2 * j]) for j in range(len(level) // 2)
                ]
            gaps.append(level[0] - coords[comp])
        weight = jnp.exp(-0.5 * (gaps[0] * gaps[0] + gaps[1] * gaps[1] + gaps[2] * gaps[2]))
        return tuple(t + g * weight for t, g in zip(total, gaps))

    zero = jnp.zeros((8, 128), f32)
    return lax.fori_loop(0, nbr_ref.shape[0], entry, (zero, zero, zero), unroll=16)


def prep_kernel(own_ref, slot_ref, pos_ref, vel_ref, nbr_ref,
                inv_ref, rank_ref, hot_ref, icnt_ref, force_ref, p8_ref, v8_ref):
    row_id = lax.broadcasted_iota(i32, (128, 128), 0)
    lane_id = lax.broadcasted_iota(i32, (128, 128), 1)
    own = [spread(own_ref[...], k, 128) for k in range(2)]
    own_t = [o.T for o in own]
    ranks = []
    for k in range(2):
        count = jnp.zeros((128, 128), i32)
        for other in range(2):
            count = count + jnp.where((own_t[other] == own[k]) & (row_id < lane_id), 1, 0)
        ranks.append(jnp.sum(count, axis=0, keepdims=True))
    rank_ref[...] = jnp.concatenate(ranks + [jnp.zeros((6, 128), i32)], axis=0)
    rank_t = [jnp.broadcast_to(r, (128, 128)).T for r in ranks]
    rows = []
    for r in range(4):
        cell = jnp.zeros((128, 128), i32)
        for k in range(2):
            cell = cell + jnp.where((own_t[k] == lane_id) & (rank_t[k] == r), row_id + 1, 0)
        rows.append(jnp.sum(cell, axis=0, keepdims=True) - 1)
    inv_ref[...] = jnp.concatenate(rows + [jnp.zeros((4, 128), i32)], axis=0)
    slots = slot_ref[...]
    count = jnp.zeros((128, 16), f32)
    want = lax.broadcasted_iota(i32, (16, 128), 0) >> 2
    for s in range(8):
        one = spread(slots, s, 128)
        hot = jnp.where((one >> 2) == row_id, 1.0, 0.0).astype(bf16)
        hot_ref[:, s * 128 : (s + 1) * 128] = hot
        match = jnp.where((spread(slots, s, 16) & 3) == want, 1.0, 0.0).astype(bf16)
        count = count + lax.dot_general(
            hot, match, (((1,), (1,)), ((), ())), preferred_element_type=f32
        )
    icnt_ref[...] = 1.0 / jnp.maximum(count, 1.0)
    for c in range(3):
        for s in range(8):
            p8_ref[c, s : s + 1, :] = pos_ref[c : c + 1, s * 128 : (s + 1) * 128]
            v8_ref[c, s : s + 1, :] = vel_ref[c : c + 1, s * 128 : (s + 1) * 128]
    total = pair_sum([p8_ref[0], p8_ref[1], p8_ref[2]], nbr_ref)
    for c in range(3):
        force_ref[c] = total[c]


def md_kernel(arr_ref, p8_ref, v8_ref, force_ref, nbr_ref, slot_ref, hot_ref, icnt_ref,
              pos_ref, vel_ref, mom_ref):
    table = arr_ref[...].T
    slots = slot_ref[...]
    source = slots >> 2
    which = slots & 3
    target = []
    for c in range(4):
        value = lanes(spread(table, c), source)
        for r in range(1, 4):
            value = jnp.where(which == r, lanes(spread(table, r * 4 + c), source), value)
        target.append(value)
    drag = friction * target[3]
    pos = [p8_ref[c] for c in range(3)]
    vel = [v8_ref[c] for c in range(3)]
    for step in range(MD_STEPS):
        pair = [force_ref[c] for c in range(3)] if step == 0 else pair_sum(pos, nbr_ref)
        for c in range(3):
            force = pair_strength * pair[c] + drag * (target[c] - vel[c])
            vel[c] = vel[c] + time_step * force
            pos[c] = pos[c] + time_step * vel[c]
    speed = vel[0] * vel[0] + vel[1] * vel[1] + vel[2] * vel[2]
    data = vel + [speed]
    row_id = lax.broadcasted_iota(i32, (16, 128), 0)
    comp = row_id & 3
    sums = jnp.zeros((128, 16), f32)
    for s in range(8):
        value = spread(data[0], s, 16)
        for c in range(1, 4):
            value = jnp.where(comp == c, spread(data[c], s, 16), value)
        value = jnp.where((spread(slots, s, 16) & 3) == (row_id >> 2), value, 0.0)
        hot = hot_ref[:, s * 128 : (s + 1) * 128]
        for part in range(3):
            piece = value.astype(bf16)
            value = value - piece.astype(f32)
            sums = sums + lax.dot_general(
                hot, piece, (((1,), (1,)), ((), ())), preferred_element_type=f32
            )
    mom_ref[...] = jnp.zeros((128, 128), f32)
    mom_ref[:, :16] = sums * icnt_ref[...]
    for c in range(3):
        for s in range(8):
            pos_ref[c : c + 1, s * 128 : (s + 1) * 128] = pos[c][s : s + 1, :]
            vel_ref[c : c + 1, s * 128 : (s + 1) * 128] = vel[c][s : s + 1, :]


def cell_kernel(back_ref, own_ref, rank_ref, out_ref):
    table = back_ref[...].T[:16, :]
    which = lax.broadcasted_iota(i32, (16, 128), 0) >> 2
    total = jnp.zeros((16, 128), f32)
    for k in range(2):
        picked = lanes(table, spread(own_ref[...], k, 16))
        total = total + jnp.where(spread(rank_ref[...], k, 16) == which, picked, 0.0)
    cell = total[0:4] + total[4:8] + total[8:12] + total[12:16]
    out_ref[:, 0, :] = cell[:, :64]
    out_ref[:, 1, :] = cell[:, 64:]


def shape(*dims, dtype=f32):
    return jax.ShapeDtypeStruct(dims, dtype)


def exchange(rows):
    return lax.all_to_all(rows, ("slab", "md"), split_axis=0, concat_axis=0, tiled=True)


near_pairs = [(i, i ^ 1) for i in range(32)]
far_pairs = [(i, (i + 1) % 32 if i % 2 else (i - 1) % 32) for i in range(32)]


def on_device(populations, relax, owners, positions, velocities, neighbours, atom_slots):
    own = owners.reshape(128, 2).T
    slots = atom_slots.reshape(8, 128)
    nbr = neighbours.reshape(8, 128, 64).transpose(2, 0, 1)
    inv, rank, hot, icnt, force, p8, v8 = pl.pallas_call(
        prep_kernel,
        out_shape=(
            shape(8, 128, dtype=i32),
            shape(8, 128, dtype=i32),
            shape(128, 1024, dtype=bf16),
            shape(128, 16),
            shape(3, 8, 128),
            shape(3, 8, 128),
            shape(3, 8, 128),
        ),
        name="prep",
    )(own, slots, positions, velocities, nbr)
    post, up, down, low, high = pl.pallas_call(
        first_kernel,
        out_shape=(
            shape(19, 2, 64, 128),
            shape(20, 64, 128),
            shape(20, 64, 128),
            shape(20, 2, 8, 128),
            shape(20, 2, 8, 128),
        ),
        name="first",
    )(populations, relax)
    below = lax.ppermute(down, "slab", far_pairs)
    above = lax.ppermute(up, "slab", near_pairs)
    from_low = lax.ppermute(high, "md", [(i, (i + 1) % 4) for i in range(4)])
    from_high = lax.ppermute(low, "md", [((i + 1) % 4, i) for i in range(4)])
    post_edge, up_edge, down_edge, relax_edge = pl.pallas_call(
        edge_kernel,
        out_shape=(
            shape(19, 2, 8, 128),
            shape(20, 8, 128),
            shape(20, 8, 128),
            shape(2, 8, 128),
        ),
        name="edge",
    )(from_low, from_high)
    below_edge = lax.ppermute(down_edge, "slab", far_pairs)
    above_edge = lax.ppermute(up_edge, "slab", near_pairs)
    scratch = [
        pltpu.VMEM((19, 2, PAD, 128), f32),
        pltpu.VMEM((5, PAD, 128), f32),
        pltpu.VMEM((5, PAD, 128), f32),
        pltpu.VMEM((len(sliding), 24, 128), f32),
        pltpu.VMEM((len(sliding), 24, 128), f32),
    ]
    post, up, down, relax_all = pl.pallas_call(
        middle_kernel,
        out_shape=(
            shape(19, 2, PAD, 128),
            shape(19, ROWS, 128),
            shape(19, ROWS, 128),
            shape(4, ROWS, 128),
        ),
        scratch_shapes=scratch + [pltpu.VMEM((2 * len(moving), 24, 128), f32)],
        name="middle",
    )(post, post_edge, below, above, below_edge, above_edge, relax, relax_edge)
    below = lax.ppermute(down, "slab", far_pairs)
    above = lax.ppermute(up, "slab", near_pairs)
    f, outgoing = pl.pallas_call(
        last_kernel,
        out_shape=(shape(19, 2, 64, 128), shape(128, 128)),
        scratch_shapes=scratch + [pltpu.VMEM((4, 128, 128), f32)],
        name="last",
    )(post, below, above, relax_all, inv)
    arrived = exchange(outgoing)
    pos_out, vel_out, moms = pl.pallas_call(
        md_kernel, out_shape=(shape(3, 1024), shape(3, 1024), shape(128, 128)), name="md"
    )(arrived, p8, v8, force, nbr, slots, hot, icnt)
    returned = exchange(moms)
    cell = pl.pallas_call(cell_kernel, out_shape=shape(4, 2, 64), name="cells")(
        returned, own, rank
    )
    return (f, pos_out, vel_out, cell)


def solution(mesh):
    return jax.shard_map(
        on_device,
        mesh=mesh,
        in_specs=(
            P(None, "slab", "md", None),
            P("slab", "md", None),
            P("slab", "md", None),
            P(None, ("slab", "md")),
            P(None, ("slab", "md")),
            P(("slab", "md"), None),
            P(("slab", "md")),
        ),
        out_specs=(
            P(None, "slab", "md", None),
            P(None, ("slab", "md")),
            P(None, ("slab", "md")),
            P(None, "slab", "md"),
        ),
        check_vma=False,
    )
```

```python
import jax
import jax.numpy as jnp
from jax import lax
from jax.experimental import pallas as pl
from jax.experimental.pallas import tpu as pltpu
from jax.sharding import PartitionSpec as P

MD_STEPS = 5
f32 = jnp.float32
i32 = jnp.int32
bf16 = jnp.bfloat16

lattice_dirs = [
    (0, 0, 0),
    (1, 0, 0),
    (-1, 0, 0),
    (0, 1, 0),
    (0, -1, 0),
    (0, 0, 1),
    (0, 0, -1),
    (1, 1, 0),
    (-1, -1, 0),
    (1, -1, 0),
    (-1, 1, 0),
    (1, 0, 1),
    (-1, 0, -1),
    (1, 0, -1),
    (-1, 0, 1),
    (0, 1, 1),
    (0, -1, -1),
    (0, 1, -1),
    (0, -1, 1),
]
lattice_weights = [1.0 / 3.0] + [1.0 / 18.0] * 6 + [1.0 / 36.0] * 12
velocity_scale = 10.0
pair_strength = 0.5
friction = 2.0
time_step = 0.1


def mirrored(direction):
    return lattice_dirs.index((direction[0], direction[1], -direction[2]))


flip = [mirrored(c) for c in lattice_dirs]
rising = [i for i, c in enumerate(lattice_dirs) if c[2] == 1]
falling = [flip[i] for i in rising]
level = [i for i, c in enumerate(lattice_dirs) if c[2] == 0]
pairs = [(1, 2), (3, 4), (5, 6)] + [(i, i + 1) for i in range(7, 19, 2)]
NEAR = 14
RELAX = 19
ROWS = 72
PAD = 88


def parity():
    return lax.axis_index("slab") & 1


def actual(index, odd):
    return jnp.where(odd == 1, flip[index], index)


def moments_of(f):
    s = {}
    for plus, minus in pairs:
        s[plus] = (f[plus] + f[minus], f[plus] - f[minus])
    density = f[0]
    for plus, _ in pairs:
        density = density + s[plus][0]
    flow = []
    for axis_id in range(3):
        total = None
        for plus, _ in pairs:
            sign = lattice_dirs[plus][axis_id]
            if sign == 0:
                continue
            term = s[plus][1]
            if total is None:
                total = term
            else:
                total = total + term if sign > 0 else total - term
        flow.append(total)
    return density, flow


def collided(f, relax, wanted):
    density, flow = moments_of(f)
    inverse = 1.0 / density
    vel = [j * inverse for j in flow]
    usq = vel[0] * vel[0] + vel[1] * vel[1] + vel[2] * vel[2]
    keep = 1.0 - relax
    gain = relax * density
    base = gain - (1.5 * gain) * usq
    result = {}
    if 0 in wanted:
        result[0] = keep * f[0] + lattice_weights[0] * base
    for plus, minus in pairs:
        if plus not in wanted and minus not in wanted:
            continue
        along = None
        for axis_id in range(3):
            sign = lattice_dirs[plus][axis_id]
            if sign != 0:
                part = vel[axis_id]
                if along is None:
                    along = part
                else:
                    along = along + part if sign > 0 else along - part
        weight = lattice_weights[plus]
        slope = (3.0 * weight) * (gain * along)
        even = weight * base + 1.5 * (along * slope)
        if plus in wanted:
            result[plus] = keep * f[plus] + (even + slope)
        if minus in wanted:
            result[minus] = keep * f[minus] + (even - slope)
    return {i: rolled(v, lattice_dirs[i][1]) for i, v in result.items()}


def rolled(block, by):
    return block if by == 0 else pltpu.roll(block, by % 128, 1)


def put(ref, where, block_id, value):
    ref[(*where, pl.ds(8 + 8 * block_id, 8), slice(None))] = value
    if block_id == 0:
        ref[(*where, pl.ds(8 + ROWS, 1), slice(None))] = value[0:1, :]
    if block_id == 8:
        ref[(*where, pl.ds(7, 1), slice(None))] = value[7:8, :]


def get(ref, where, block_id, shift):
    return ref[(*where, pl.ds(8 + 8 * block_id - shift, 8), slice(None))]


def rows_of(block_id):
    return pl.ds(8 * block_id, 8)


def send_planes(up_ref, down_ref, plane, block, post, relax):
    for k in range(5):
        up_ref[k if plane == 1 else NEAR + k, block, :] = post[rising[k]]
        down_ref[k if plane == 0 else NEAR + k, block, :] = post[falling[k]]
    near_ref = up_ref if plane == 1 else down_ref
    for k, i in enumerate(level):
        near_ref[5 + k, block, :] = post[i]
    if relax is not None:
        near_ref[RELAX, block, :] = relax


everything = set(range(19))


def first_kernel(f_ref, relax_ref, post_ref, up_ref, down_ref, low_ref, high_ref):
    odd = parity()
    for plane in range(2):
        actual_plane = jnp.where(odd == 1, 1 - plane, plane)
        for b in range(8):
            f = {i: f_ref[actual(i, odd), actual_plane, rows_of(b), :] for i in range(19)}
            relax = relax_ref[actual_plane, rows_of(b), :]
            if b in (0, 7):
                edge_ref = low_ref if b == 0 else high_ref
                for i in range(19):
                    edge_ref[i, plane] = f[i]
                edge_ref[RELAX, plane] = relax
            post = collided(f, relax, everything)
            for i in range(19):
                post_ref[i, plane, rows_of(b), :] = post[i]
            send_planes(up_ref, down_ref, plane, rows_of(b), post, relax)


def edge_kernel(low_ref, high_ref, post_ref, up_ref, down_ref, relax_ref):
    head = lax.broadcasted_iota(i32, (8, 128), 0) < 4
    for plane in range(2):
        mixed = [jnp.where(head, high_ref[i, plane], low_ref[i, plane]) for i in range(20)]
        post = collided(dict(enumerate(mixed[:19])), mixed[RELAX], everything)
        relax_ref[plane] = mixed[RELAX]
        for i in range(19):
            post_ref[i, plane] = post[i]
        send_planes(up_ref, down_ref, plane, rows_of(0), post, mixed[RELAX])


def two_steps(own, below, above, relax, second_ref, from_below_ref, from_above_ref):
    for b in range(9):
        for plane in (-1, 0, 1, 2):
            f = {}
            for i, c in enumerate(lattice_dirs):
                source = plane - c[2]
                if source in (0, 1):
                    f[i] = own(i, source, b, c[0])
                else:
                    side = below if source < 0 else above
                    if c[2] == 0:
                        j = 5 + level.index(i)
                    else:
                        j = (rising if c[2] == 1 else falling).index(i)
                        if source in (-2, 3):
                            j = NEAR + j
                    f[i] = side(j, b, c[0])
            wanted = everything
            if plane == -1:
                wanted = set(rising)
            elif plane == 2:
                wanted = set(falling)
            post = collided(f, relax(plane, b), wanted)
            for i, value in post.items():
                if plane == -1:
                    put(from_below_ref, (rising.index(i),), b, value)
                elif plane == 2:
                    put(from_above_ref, (falling.index(i),), b, value)
                else:
                    put(second_ref, (i, plane), b, value)


def streamed(second_ref, from_below_ref, from_above_ref, plane, b):
    f = {}
    for i, c in enumerate(lattice_dirs):
        source = plane - c[2]
        if source == -1:
            f[i] = get(from_below_ref, (rising.index(i),), b, c[0])
        elif source == 2:
            f[i] = get(from_above_ref, (falling.index(i),), b, c[0])
        else:
            f[i] = get(second_ref, (i, source), b, c[0])
    return f


sliding = [k for k, i in enumerate(rising + level + rising) if lattice_dirs[i][0] != 0]
moving = [i for i, c in enumerate(lattice_dirs) if c[0] != 0]


def seamed(seam_ref, slots, at):
    for slot, key in enumerate(slots):
        for part, b in enumerate((7, 8, 0)):
            seam_ref[slot, 8 * part : 8 * part + 8, :] = at(key, b)

    def read(key, b, shift, main):
        if shift == 0:
            return at(key, b)
        slot = slots.index(key)
        if b == 8:
            return seam_ref[slot, 8 - shift : 16 - shift, :]
        if b == 0 and shift == 1:
            return seam_ref[slot, 15:23, :]
        if b == 7 and shift == -1:
            return seam_ref[slot, 1:9, :]
        return main(8 * b - shift)

    return read


def reader(seam_ref, main_ref, edge_ref):
    def at(j, b):
        if edge_ref is None or b < 8:
            return main_ref[j, rows_of(b), :]
        return edge_ref[j, rows_of(0), :]

    read = seamed(seam_ref, sliding, at)
    return lambda j, b, shift: read(j, b, shift, lambda row: main_ref[j, row : row + 8, :])


def own_reader(seam_ref, main_ref, edge_ref):
    def at(key, b):
        i, plane = key
        return main_ref[i, plane, rows_of(b), :] if b < 8 else edge_ref[i, plane]

    read = seamed(seam_ref, [(i, plane) for i in moving for plane in range(2)], at)
    return lambda i, plane, b, shift: read(
        (i, plane), b, shift, lambda row: main_ref[i, plane, row : row + 8, :]
    )


def middle_kernel(post_ref, post_edge_ref, below_ref, above_ref, below_edge_ref, above_edge_ref,
                  relax_ref, relax_edge_ref,
                  third_ref, up_ref, down_ref, relax_out_ref,
                  second_ref, from_below_ref, from_above_ref, below_seam_ref, above_seam_ref,
                  own_seam_ref):
    odd = parity()
    own = own_reader(own_seam_ref, post_ref, post_edge_ref)
    below = reader(below_seam_ref, below_ref, below_edge_ref)
    above = reader(above_seam_ref, above_ref, above_edge_ref)
    for b in range(8):
        relax_out_ref[0, rows_of(b), :] = below_ref[RELAX, rows_of(b), :]
        relax_out_ref[3, rows_of(b), :] = above_ref[RELAX, rows_of(b), :]
        for plane in range(2):
            relax_out_ref[1 + plane, rows_of(b), :] = relax_ref[
                jnp.where(odd == 1, 1 - plane, plane), rows_of(b), :
            ]
    relax_out_ref[0, rows_of(8), :] = below_edge_ref[RELAX, rows_of(0), :]
    relax_out_ref[3, rows_of(8), :] = above_edge_ref[RELAX, rows_of(0), :]
    for plane in range(2):
        relax_out_ref[1 + plane, rows_of(8), :] = relax_edge_ref[plane]

    def relax(plane, b):
        return relax_out_ref[1 + plane, rows_of(b), :]

    two_steps(own, below, above, relax, second_ref, from_below_ref, from_above_ref)
    for b in range(9):
        for plane in range(2):
            f = streamed(second_ref, from_below_ref, from_above_ref, plane, b)
            post = collided(f, relax(plane, b), everything)
            for i in range(19):
                put(third_ref, (i, plane), b, post[i])
            send_planes(up_ref, down_ref, plane, rows_of(b), post, None)


def last_kernel(post_ref, below_ref, above_ref, relax_ref, inv_ref,
                f_ref, out_ref,
                second_ref, from_below_ref, from_above_ref, below_seam_ref, above_seam_ref,
                flow_ref):
    odd = parity()
    below = reader(below_seam_ref, below_ref, None)
    above = reader(above_seam_ref, above_ref, None)

    def own(i, plane, b, shift):
        return get(post_ref, (i, plane), b, shift)

    def relax(plane, b):
        return relax_ref[1 + plane, rows_of(b), :]

    two_steps(own, below, above, relax, second_ref, from_below_ref, from_above_ref)
    upward = jnp.where(odd == 1, -velocity_scale / 128.0, velocity_scale / 128.0)
    for plane in range(2):
        actual_plane = jnp.where(odd == 1, 1 - plane, plane)
        for b in range(8):
            f = streamed(second_ref, from_below_ref, from_above_ref, plane, b)
            for i in range(19):
                f_ref[actual(i, odd), actual_plane, rows_of(b), :] = f[i]
            density, flow = moments_of(f)
            inverse = 1.0 / density
            where = pl.ds(pl.multiple_of(actual_plane * 64 + 8 * b, 8), 8)
            flow_ref[0, where, :] = flow[0] * inverse * (velocity_scale / 128.0)
            flow_ref[1, where, :] = flow[1] * inverse * (velocity_scale / 128.0)
            flow_ref[2, where, :] = flow[2] * inverse * upward
            flow_ref[3, where, :] = density * (1.0 / 128.0)
    means = [jnp.sum(flow_ref[c].T, axis=0, keepdims=True) for c in range(4)]
    packed = jnp.concatenate(means * 4, axis=0)
    inv16 = jnp.concatenate(
        [jnp.broadcast_to(inv_ref[r : r + 1, :], (4, 128)) for r in range(4)], axis=0
    )
    picked = jnp.where(inv16 >= 0, lanes(packed, jnp.maximum(inv16, 0)), 0.0)
    out_ref[...] = jnp.concatenate([picked, jnp.zeros((112, 128), f32)], axis=0).T


def lanes(table, index):
    return jnp.take_along_axis(table, index, axis=1, mode="promise_in_bounds")


def spread(block, index, rows=8):
    return jnp.broadcast_to(block[index : index + 1, :], (rows, 128))


def pair_sum(coords, nbr_ref):
    tables = [[spread(comp, chunk) for chunk in range(8)] for comp in coords]

    def entry(k, total):
        index = nbr_ref[k]
        low = index & 127
        bits = [(index & mask) != 0 for mask in (128, 256, 512)]
        gaps = []
        for comp in range(3):
            level = [lanes(table, low) for table in tables[comp]]
            for bit in bits:
                level = [
                    jnp.where(bit, level[2 * j + 1], level[2 * j]) for j in range(len(level) // 2)
                ]
            gaps.append(level[0] - coords[comp])
        weight = jnp.exp(-0.5 * (gaps[0] * gaps[0] + gaps[1] * gaps[1] + gaps[2] * gaps[2]))
        return tuple(t + g * weight for t, g in zip(total, gaps))

    zero = jnp.zeros((8, 128), f32)
    return lax.fori_loop(0, nbr_ref.shape[0], entry, (zero, zero, zero), unroll=16)


def prep_kernel(own_ref, slot_ref, pos_ref, vel_ref, nbr_ref,
                inv_ref, rank_ref, hot_ref, icnt_ref, force_ref, p8_ref, v8_ref):
    row_id = lax.broadcasted_iota(i32, (128, 128), 0)
    lane_id = lax.broadcasted_iota(i32, (128, 128), 1)
    own = [spread(own_ref[...], k, 128) for k in range(2)]
    own_t = [o.T for o in own]
    ranks = []
    for k in range(2):
        count = jnp.zeros((128, 128), i32)
        for other in range(2):
            count = count + jnp.where((own_t[other] == own[k]) & (row_id < lane_id), 1, 0)
        ranks.append(jnp.sum(count, axis=0, keepdims=True))
    rank_ref[...] = jnp.concatenate(ranks + [jnp.zeros((6, 128), i32)], axis=0)
    rank_t = [jnp.broadcast_to(r, (128, 128)).T for r in ranks]
    rows = []
    for r in range(4):
        cell = jnp.zeros((128, 128), i32)
        for k in range(2):
            cell = cell + jnp.where((own_t[k] == lane_id) & (rank_t[k] == r), row_id + 1, 0)
        rows.append(jnp.sum(cell, axis=0, keepdims=True) - 1)
    inv_ref[...] = jnp.concatenate(rows + [jnp.zeros((4, 128), i32)], axis=0)
    slots = slot_ref[...]
    count = jnp.zeros((128, 16), f32)
    want = lax.broadcasted_iota(i32, (16, 128), 0) >> 2
    for s in range(8):
        one = spread(slots, s, 128)
        hot = jnp.where((one >> 2) == row_id, 1.0, 0.0).astype(bf16)
        hot_ref[:, s * 128 : (s + 1) * 128] = hot
        match = jnp.where((spread(slots, s, 16) & 3) == want, 1.0, 0.0).astype(bf16)
        count = count + lax.dot_general(
            hot, match, (((1,), (1,)), ((), ())), preferred_element_type=f32
        )
    icnt_ref[...] = 1.0 / jnp.maximum(count, 1.0)
    for c in range(3):
        for s in range(8):
            p8_ref[c, s : s + 1, :] = pos_ref[c : c + 1, s * 128 : (s + 1) * 128]
            v8_ref[c, s : s + 1, :] = vel_ref[c : c + 1, s * 128 : (s + 1) * 128]
    total = pair_sum([p8_ref[0], p8_ref[1], p8_ref[2]], nbr_ref)
    for c in range(3):
        force_ref[c] = total[c]


def md_kernel(arr_ref, p8_ref, v8_ref, force_ref, nbr_ref, slot_ref, hot_ref, icnt_ref,
              pos_ref, vel_ref, mom_ref):
    table = arr_ref[...].T
    slots = slot_ref[...]
    source = slots >> 2
    which = slots & 3
    target = []
    for c in range(4):
        value = lanes(spread(table, c), source)
        for r in range(1, 4):
            value = jnp.where(which == r, lanes(spread(table, r * 4 + c), source), value)
        target.append(value)
    drag = friction * target[3]
    pos = [p8_ref[c] for c in range(3)]
    vel = [v8_ref[c] for c in range(3)]
    for step in range(MD_STEPS):
        pair = [force_ref[c] for c in range(3)] if step == 0 else pair_sum(pos, nbr_ref)
        for c in range(3):
            force = pair_strength * pair[c] + drag * (target[c] - vel[c])
            vel[c] = vel[c] + time_step * force
            pos[c] = pos[c] + time_step * vel[c]
    speed = vel[0] * vel[0] + vel[1] * vel[1] + vel[2] * vel[2]
    data = vel + [speed]
    row_id = lax.broadcasted_iota(i32, (16, 128), 0)
    comp = row_id & 3
    sums = jnp.zeros((128, 16), f32)
    for s in range(8):
        value = spread(data[0], s, 16)
        for c in range(1, 4):
            value = jnp.where(comp == c, spread(data[c], s, 16), value)
        value = jnp.where((spread(slots, s, 16) & 3) == (row_id >> 2), value, 0.0)
        hot = hot_ref[:, s * 128 : (s + 1) * 128]
        for part in range(3):
            piece = value.astype(bf16)
            value = value - piece.astype(f32)
            sums = sums + lax.dot_general(
                hot, piece, (((1,), (1,)), ((), ())), preferred_element_type=f32
            )
    mom_ref[...] = jnp.zeros((128, 128), f32)
    mom_ref[:, :16] = sums * icnt_ref[...]
    for c in range(3):
        for s in range(8):
            pos_ref[c : c + 1, s * 128 : (s + 1) * 128] = pos[c][s : s + 1, :]
            vel_ref[c : c + 1, s * 128 : (s + 1) * 128] = vel[c][s : s + 1, :]


def cell_kernel(back_ref, own_ref, rank_ref, out_ref):
    table = back_ref[...].T[:16, :]
    which = lax.broadcasted_iota(i32, (16, 128), 0) >> 2
    total = jnp.zeros((16, 128), f32)
    for k in range(2):
        picked = lanes(table, spread(own_ref[...], k, 16))
        total = total + jnp.where(spread(rank_ref[...], k, 16) == which, picked, 0.0)
    cell = total[0:4] + total[4:8] + total[8:12] + total[12:16]
    out_ref[:, 0, :] = cell[:, :64]
    out_ref[:, 1, :] = cell[:, 64:]


room = pltpu.CompilerParams(vmem_limit_bytes=16 << 20)


def shape(*dims, dtype=f32):
    return jax.ShapeDtypeStruct(dims, dtype)


def exchange(rows):
    return lax.all_to_all(rows, ("slab", "md"), split_axis=0, concat_axis=0, tiled=True)


near_pairs = [(i, i ^ 1) for i in range(32)]
far_pairs = [(i, (i + 1) % 32 if i % 2 else (i - 1) % 32) for i in range(32)]


def on_device(populations, relax, owners, positions, velocities, neighbours, atom_slots):
    own = owners.reshape(128, 2).T
    slots = atom_slots.reshape(8, 128)
    nbr = neighbours.reshape(8, 128, 64).transpose(2, 0, 1)
    inv, rank, hot, icnt, force, p8, v8 = pl.pallas_call(
        prep_kernel,
        out_shape=(
            shape(8, 128, dtype=i32),
            shape(8, 128, dtype=i32),
            shape(128, 1024, dtype=bf16),
            shape(128, 16),
            shape(3, 8, 128),
            shape(3, 8, 128),
            shape(3, 8, 128),
        ),
        name="prep", compiler_params=room,
    )(own, slots, positions, velocities, nbr)
    post, up, down, low, high = pl.pallas_call(
        first_kernel,
        out_shape=(
            shape(19, 2, 64, 128),
            shape(20, 64, 128),
            shape(20, 64, 128),
            shape(20, 2, 8, 128),
            shape(20, 2, 8, 128),
        ),
        name="first", compiler_params=room,
    )(populations, relax)
    below = lax.ppermute(down, "slab", far_pairs)
    above = lax.ppermute(up, "slab", near_pairs)
    from_low = lax.ppermute(high, "md", [(i, (i + 1) % 4) for i in range(4)])
    from_high = lax.ppermute(low, "md", [((i + 1) % 4, i) for i in range(4)])
    post_edge, up_edge, down_edge, relax_edge = pl.pallas_call(
        edge_kernel,
        out_shape=(
            shape(19, 2, 8, 128),
            shape(20, 8, 128),
            shape(20, 8, 128),
            shape(2, 8, 128),
        ),
        name="edge", compiler_params=room,
    )(from_low, from_high)
    below_edge = lax.ppermute(down_edge, "slab", far_pairs)
    above_edge = lax.ppermute(up_edge, "slab", near_pairs)
    scratch = [
        pltpu.VMEM((19, 2, PAD, 128), f32),
        pltpu.VMEM((5, PAD, 128), f32),
        pltpu.VMEM((5, PAD, 128), f32),
        pltpu.VMEM((len(sliding), 24, 128), f32),
        pltpu.VMEM((len(sliding), 24, 128), f32),
    ]
    post, up, down, relax_all = pl.pallas_call(
        middle_kernel,
        out_shape=(
            shape(19, 2, PAD, 128),
            shape(19, ROWS, 128),
            shape(19, ROWS, 128),
            shape(4, ROWS, 128),
        ),
        scratch_shapes=scratch + [pltpu.VMEM((2 * len(moving), 24, 128), f32)],
        name="middle", compiler_params=room,
    )(post, post_edge, below, above, below_edge, above_edge, relax, relax_edge)
    below = lax.ppermute(down, "slab", far_pairs)
    above = lax.ppermute(up, "slab", near_pairs)
    f, outgoing = pl.pallas_call(
        last_kernel,
        out_shape=(shape(19, 2, 64, 128), shape(128, 128)),
        scratch_shapes=scratch + [pltpu.VMEM((4, 128, 128), f32)],
        name="last", compiler_params=room,
    )(post, below, above, relax_all, inv)
    arrived = exchange(outgoing)
    pos_out, vel_out, moms = pl.pallas_call(
        md_kernel, out_shape=(shape(3, 1024), shape(3, 1024), shape(128, 128)), name="md", compiler_params=room
    )(arrived, p8, v8, force, nbr, slots, hot, icnt)
    returned = exchange(moms)
    cell = pl.pallas_call(cell_kernel, out_shape=shape(4, 2, 64), name="cells", compiler_params=room)(
        returned, own, rank
    )
    return (f, pos_out, vel_out, cell)


def solution(mesh):
    return jax.shard_map(
        on_device,
        mesh=mesh,
        in_specs=(
            P(None, "slab", "md", None),
            P("slab", "md", None),
            P("slab", "md", None),
            P(None, ("slab", "md")),
            P(None, ("slab", "md")),
            P(("slab", "md"), None),
            P(("slab", "md")),
        ),
        out_specs=(
            P(None, "slab", "md", None),
            P(None, ("slab", "md")),
            P(None, ("slab", "md")),
            P(None, "slab", "md"),
        ),
        check_vma=False,
    )
```

```python
import jax
import jax.numpy as jnp
from jax import lax
from jax.experimental import pallas as pl
from jax.experimental.pallas import tpu as pltpu
from jax.sharding import PartitionSpec as P

MD_STEPS = 5
f32 = jnp.float32
i32 = jnp.int32
bf16 = jnp.bfloat16

lattice_dirs = [
    (0, 0, 0),
    (1, 0, 0),
    (-1, 0, 0),
    (0, 1, 0),
    (0, -1, 0),
    (0, 0, 1),
    (0, 0, -1),
    (1, 1, 0),
    (-1, -1, 0),
    (1, -1, 0),
    (-1, 1, 0),
    (1, 0, 1),
    (-1, 0, -1),
    (1, 0, -1),
    (-1, 0, 1),
    (0, 1, 1),
    (0, -1, -1),
    (0, 1, -1),
    (0, -1, 1),
]
lattice_weights = [1.0 / 3.0] + [1.0 / 18.0] * 6 + [1.0 / 36.0] * 12
velocity_scale = 10.0
pair_strength = 0.5
friction = 2.0
time_step = 0.1


def mirrored(direction):
    return lattice_dirs.index((direction[0], direction[1], -direction[2]))


flip = [mirrored(c) for c in lattice_dirs]
rising = [i for i, c in enumerate(lattice_dirs) if c[2] == 1]
falling = [flip[i] for i in rising]
level = [i for i, c in enumerate(lattice_dirs) if c[2] == 0]
pairs = [(1, 2), (3, 4), (5, 6)] + [(i, i + 1) for i in range(7, 19, 2)]
NEAR = 14
RELAX = 19
ROWS = 72
PAD = 88


def parity():
    return lax.axis_index("slab") & 1


def actual(index, odd):
    return jnp.where(odd == 1, flip[index], index)


def moments_of(f):
    s = {}
    for plus, minus in pairs:
        s[plus] = (f[plus] + f[minus], f[plus] - f[minus])
    density = f[0]
    for plus, _ in pairs:
        density = density + s[plus][0]
    flow = []
    for axis_id in range(3):
        total = None
        for plus, _ in pairs:
            sign = lattice_dirs[plus][axis_id]
            if sign == 0:
                continue
            term = s[plus][1]
            if total is None:
                total = term
            else:
                total = total + term if sign > 0 else total - term
        flow.append(total)
    return density, flow


def collided(f, relax, wanted):
    density, flow = moments_of(f)
    inverse = 1.0 / density
    vel = [j * inverse for j in flow]
    usq = vel[0] * vel[0] + vel[1] * vel[1] + vel[2] * vel[2]
    keep = 1.0 - relax
    gain = relax * density
    base = gain - (1.5 * gain) * usq
    result = {}
    if 0 in wanted:
        result[0] = keep * f[0] + lattice_weights[0] * base
    for plus, minus in pairs:
        if plus not in wanted and minus not in wanted:
            continue
        along = None
        for axis_id in range(3):
            sign = lattice_dirs[plus][axis_id]
            if sign != 0:
                part = vel[axis_id]
                if along is None:
                    along = part
                else:
                    along = along + part if sign > 0 else along - part
        weight = lattice_weights[plus]
        slope = (3.0 * weight) * (gain * along)
        even = weight * base + 1.5 * (along * slope)
        if plus in wanted:
            result[plus] = keep * f[plus] + (even + slope)
        if minus in wanted:
            result[minus] = keep * f[minus] + (even - slope)
    return {i: rolled(v, lattice_dirs[i][1]) for i, v in result.items()}


def rolled(block, by):
    return block if by == 0 else pltpu.roll(block, by % 128, 1)


def put(ref, where, block_id, value):
    ref[(*where, pl.ds(8 + 8 * block_id, 8), slice(None))] = value
    if block_id == 0:
        ref[(*where, pl.ds(8 + ROWS, 1), slice(None))] = value[0:1, :]
    if block_id == 8:
        ref[(*where, pl.ds(7, 1), slice(None))] = value[7:8, :]


def get(ref, where, block_id, shift):
    return ref[(*where, pl.ds(8 + 8 * block_id - shift, 8), slice(None))]


def rows_of(block_id):
    return pl.ds(8 * block_id, 8)


def send_planes(up_ref, down_ref, plane, block, post, relax):
    for k in range(5):
        up_ref[k if plane == 1 else NEAR + k, block, :] = post[rising[k]]
        down_ref[k if plane == 0 else NEAR + k, block, :] = post[falling[k]]
    near_ref = up_ref if plane == 1 else down_ref
    for k, i in enumerate(level):
        near_ref[5 + k, block, :] = post[i]
    if relax is not None:
        near_ref[RELAX, block, :] = relax


everything = set(range(19))


def load_kernel(f_ref, relax_ref, low_ref, high_ref, f_out_ref, relax_out_ref, sems):
    moves = []
    for edge_ref, row in ((low_ref, 0), (high_ref, 56)):
        rows = pl.ds(row, 8)
        moves.append((f_ref.at[:, :, rows, :], edge_ref.at[0:19]))
        moves.append((relax_ref.at[:, rows, :], edge_ref.at[RELAX]))
    moves.append((relax_ref, relax_out_ref))
    for part in range(4):
        some = slice(5 * part, min(5 * part + 5, 19))
        moves.append((f_ref.at[some], f_out_ref.at[some]))
    copies = [pltpu.make_async_copy(*move, sems.at[n]) for n, move in enumerate(moves)]
    for copy in copies:
        copy.start()
    for copy in copies:
        copy.wait()


def first_kernel(f_ref, relax_ref, post_ref, up_ref, down_ref):
    odd = parity()
    for plane in range(2):
        actual_plane = jnp.where(odd == 1, 1 - plane, plane)
        for b in range(8):
            f = {i: f_ref[actual(i, odd), actual_plane, rows_of(b), :] for i in range(19)}
            relax = relax_ref[actual_plane, rows_of(b), :]
            post = collided(f, relax, everything)
            for i in range(19):
                post_ref[i, plane, rows_of(b), :] = post[i]
            send_planes(up_ref, down_ref, plane, rows_of(b), post, relax)


def edge_kernel(low_ref, high_ref, post_ref, up_ref, down_ref, relax_ref):
    odd = parity()
    head = lax.broadcasted_iota(i32, (8, 128), 0) < 4
    for plane in range(2):
        actual_plane = jnp.where(odd == 1, 1 - plane, plane)
        mixed = []
        for i in range(20):
            j = actual(i, odd) if i < 19 else i
            mixed.append(jnp.where(head, high_ref[j, actual_plane], low_ref[j, actual_plane]))
        post = collided(dict(enumerate(mixed[:19])), mixed[RELAX], everything)
        relax_ref[plane] = mixed[RELAX]
        for i in range(19):
            post_ref[i, plane] = post[i]
        send_planes(up_ref, down_ref, plane, rows_of(0), post, mixed[RELAX])


def two_steps(own, below, above, relax, second_ref, from_below_ref, from_above_ref):
    for b in range(9):
        for plane in (-1, 0, 1, 2):
            f = {}
            for i, c in enumerate(lattice_dirs):
                source = plane - c[2]
                if source in (0, 1):
                    f[i] = own(i, source, b, c[0])
                else:
                    side = below if source < 0 else above
                    if c[2] == 0:
                        j = 5 + level.index(i)
                    else:
                        j = (rising if c[2] == 1 else falling).index(i)
                        if source in (-2, 3):
                            j = NEAR + j
                    f[i] = side(j, b, c[0])
            wanted = everything
            if plane == -1:
                wanted = set(rising)
            elif plane == 2:
                wanted = set(falling)
            post = collided(f, relax(plane, b), wanted)
            for i, value in post.items():
                if plane == -1:
                    put(from_below_ref, (rising.index(i),), b, value)
                elif plane == 2:
                    put(from_above_ref, (falling.index(i),), b, value)
                else:
                    put(second_ref, (i, plane), b, value)


def streamed(second_ref, from_below_ref, from_above_ref, plane, b):
    f = {}
    for i, c in enumerate(lattice_dirs):
        source = plane - c[2]
        if source == -1:
            f[i] = get(from_below_ref, (rising.index(i),), b, c[0])
        elif source == 2:
            f[i] = get(from_above_ref, (falling.index(i),), b, c[0])
        else:
            f[i] = get(second_ref, (i, source), b, c[0])
    return f


sliding = [k for k, i in enumerate(rising + level + rising) if lattice_dirs[i][0] != 0]
moving = [i for i, c in enumerate(lattice_dirs) if c[0] != 0]


def seamed(seam_ref, slots, at):
    for slot, key in enumerate(slots):
        for part, b in enumerate((7, 8, 0)):
            seam_ref[slot, 8 * part : 8 * part + 8, :] = at(key, b)

    def read(key, b, shift, main):
        if shift == 0:
            return at(key, b)
        slot = slots.index(key)
        if b == 8:
            return seam_ref[slot, 8 - shift : 16 - shift, :]
        if b == 0 and shift == 1:
            return seam_ref[slot, 15:23, :]
        if b == 7 and shift == -1:
            return seam_ref[slot, 1:9, :]
        return main(8 * b - shift)

    return read


def reader(seam_ref, main_ref, edge_ref):
    def at(j, b):
        if edge_ref is None or b < 8:
            return main_ref[j, rows_of(b), :]
        return edge_ref[j, rows_of(0), :]

    read = seamed(seam_ref, sliding, at)
    return lambda j, b, shift: read(j, b, shift, lambda row: main_ref[j, row : row + 8, :])


def own_reader(seam_ref, main_ref, edge_ref):
    def at(key, b):
        i, plane = key
        return main_ref[i, plane, rows_of(b), :] if b < 8 else edge_ref[i, plane]

    read = seamed(seam_ref, [(i, plane) for i in moving for plane in range(2)], at)
    return lambda i, plane, b, shift: read(
        (i, plane), b, shift, lambda row: main_ref[i, plane, row : row + 8, :]
    )


def middle_kernel(post_ref, post_edge_ref, below_ref, above_ref, below_edge_ref, above_edge_ref,
                  relax_ref, relax_edge_ref,
                  third_ref, up_ref, down_ref, relax_out_ref,
                  second_ref, from_below_ref, from_above_ref, below_seam_ref, above_seam_ref,
                  own_seam_ref):
    odd = parity()
    own = own_reader(own_seam_ref, post_ref, post_edge_ref)
    below = reader(below_seam_ref, below_ref, below_edge_ref)
    above = reader(above_seam_ref, above_ref, above_edge_ref)
    for b in range(8):
        relax_out_ref[0, rows_of(b), :] = below_ref[RELAX, rows_of(b), :]
        relax_out_ref[3, rows_of(b), :] = above_ref[RELAX, rows_of(b), :]
        for plane in range(2):
            relax_out_ref[1 + plane, rows_of(b), :] = relax_ref[
                jnp.where(odd == 1, 1 - plane, plane), rows_of(b), :
            ]
    relax_out_ref[0, rows_of(8), :] = below_edge_ref[RELAX, rows_of(0), :]
    relax_out_ref[3, rows_of(8), :] = above_edge_ref[RELAX, rows_of(0), :]
    for plane in range(2):
        relax_out_ref[1 + plane, rows_of(8), :] = relax_edge_ref[plane]

    def relax(plane, b):
        return relax_out_ref[1 + plane, rows_of(b), :]

    two_steps(own, below, above, relax, second_ref, from_below_ref, from_above_ref)
    for b in range(9):
        for plane in range(2):
            f = streamed(second_ref, from_below_ref, from_above_ref, plane, b)
            post = collided(f, relax(plane, b), everything)
            for i in range(19):
                put(third_ref, (i, plane), b, post[i])
            send_planes(up_ref, down_ref, plane, rows_of(b), post, None)


def last_kernel(post_ref, below_ref, above_ref, relax_ref, inv_ref,
                f_ref, out_ref,
                second_ref, from_below_ref, from_above_ref, below_seam_ref, above_seam_ref,
                flow_ref):
    odd = parity()
    below = reader(below_seam_ref, below_ref, None)
    above = reader(above_seam_ref, above_ref, None)

    def own(i, plane, b, shift):
        return get(post_ref, (i, plane), b, shift)

    def relax(plane, b):
        return relax_ref[1 + plane, rows_of(b), :]

    two_steps(own, below, above, relax, second_ref, from_below_ref, from_above_ref)
    upward = jnp.where(odd == 1, -velocity_scale / 128.0, velocity_scale / 128.0)
    for plane in range(2):
        actual_plane = jnp.where(odd == 1, 1 - plane, plane)
        for b in range(8):
            f = streamed(second_ref, from_below_ref, from_above_ref, plane, b)
            for i in range(19):
                f_ref[actual(i, odd), actual_plane, rows_of(b), :] = f[i]
            density, flow = moments_of(f)
            inverse = 1.0 / density
            where = pl.ds(pl.multiple_of(actual_plane * 64 + 8 * b, 8), 8)
            flow_ref[0, where, :] = flow[0] * inverse * (velocity_scale / 128.0)
            flow_ref[1, where, :] = flow[1] * inverse * (velocity_scale / 128.0)
            flow_ref[2, where, :] = flow[2] * inverse * upward
            flow_ref[3, where, :] = density * (1.0 / 128.0)
    means = [jnp.sum(flow_ref[c].T, axis=0, keepdims=True) for c in range(4)]
    packed = jnp.concatenate(means * 4, axis=0)
    inv16 = jnp.concatenate(
        [jnp.broadcast_to(inv_ref[r : r + 1, :], (4, 128)) for r in range(4)], axis=0
    )
    picked = jnp.where(inv16 >= 0, lanes(packed, jnp.maximum(inv16, 0)), 0.0)
    out_ref[...] = jnp.concatenate([picked, jnp.zeros((112, 128), f32)], axis=0).T


def lanes(table, index):
    return jnp.take_along_axis(table, index, axis=1, mode="promise_in_bounds")


def spread(block, index, rows=8):
    return jnp.broadcast_to(block[index : index + 1, :], (rows, 128))


def lookup(tables, index):
    low = index & 127
    found = [[lanes(chunk, low) for chunk in table] for table in tables]
    for mask in (128, 256, 512):
        bit = (index & mask) != 0
        found = [
            [jnp.where(bit, f[2 * j + 1], f[2 * j]) for j in range(len(f) // 2)] for f in found
        ]
    return [f[0] for f in found]


def chunks(block):
    return [spread(block, chunk) for chunk in range(8)]


def pull(total, near, here):
    gaps = [n - h for n, h in zip(near, here)]
    weight = jnp.exp(-0.5 * (gaps[0] * gaps[0] + gaps[1] * gaps[1] + gaps[2] * gaps[2]))
    return tuple(t + g * weight for t, g in zip(total, gaps))


def over_list(entry, start):
    return lax.fori_loop(0, 64, entry, start, unroll=16)


def blank():
    return tuple(jnp.zeros((8, 128), f32) for _ in range(3))


def prep_kernel(own_in_ref, slot_ref, pos_ref, vel_ref, nbr_ref,
                own_ref, inv_ref, rank_ref, hot_ref, icnt_ref, force_ref, p8_ref, v8_ref,
                list_ref, near_ref, drift_ref):
    for k in range(2):
        for z in range(2):
            own_ref[k : k + 1, z * 64 : (z + 1) * 64] = own_in_ref[z, k : k + 1, :]
    own_ref[2:8, :] = jnp.zeros((6, 128), i32)
    row_id = lax.broadcasted_iota(i32, (128, 128), 0)
    lane_id = lax.broadcasted_iota(i32, (128, 128), 1)
    own = [spread(own_ref[...], k, 128) for k in range(2)]
    own_t = [o.T for o in own]
    ranks = []
    for k in range(2):
        count = jnp.zeros((128, 128), i32)
        for other in range(2):
            count = count + jnp.where((own_t[other] == own[k]) & (row_id < lane_id), 1, 0)
        ranks.append(jnp.sum(count, axis=0, keepdims=True))
    rank_ref[...] = jnp.concatenate(ranks + [jnp.zeros((6, 128), i32)], axis=0)
    rank_t = [jnp.broadcast_to(r, (128, 128)).T for r in ranks]
    rows = []
    for r in range(4):
        cell = jnp.zeros((128, 128), i32)
        for k in range(2):
            cell = cell + jnp.where((own_t[k] == lane_id) & (rank_t[k] == r), row_id + 1, 0)
        rows.append(jnp.sum(cell, axis=0, keepdims=True) - 1)
    inv_ref[...] = jnp.concatenate(rows + [jnp.zeros((4, 128), i32)], axis=0)
    slots = slot_ref[...]
    count = jnp.zeros((128, 16), f32)
    want = lax.broadcasted_iota(i32, (16, 128), 0) >> 2
    for s in range(8):
        one = spread(slots, s, 128)
        hot = jnp.where((one >> 2) == row_id, 1.0, 0.0).astype(bf16)
        hot_ref[:, s * 128 : (s + 1) * 128] = hot
        match = jnp.where((spread(slots, s, 16) & 3) == want, 1.0, 0.0).astype(bf16)
        count = count + lax.dot_general(
            hot, match, (((1,), (1,)), ((), ())), preferred_element_type=f32
        )
    icnt_ref[...] = 1.0 / jnp.maximum(count, 1.0)
    for c in range(3):
        for s in range(8):
            p8_ref[c, s : s + 1, :] = pos_ref[c : c + 1, s * 128 : (s + 1) * 128]
            v8_ref[c, s : s + 1, :] = vel_ref[c : c + 1, s * 128 : (s + 1) * 128]
    for k in range(8):
        for part in range(8):
            list_ref[8 * k : 8 * k + 8, part, :] = nbr_ref[
                8 * k : 8 * k + 8, part * 128 : (part + 1) * 128
            ]
    here = [p8_ref[c] for c in range(3)]
    tables = [chunks(h) for h in here]

    def positions(k, total):
        near = lookup(tables, list_ref[k])
        for c in range(3):
            near_ref[k, c] = near[c]
        return pull(total, near, here)

    total = over_list(positions, blank())
    for c in range(3):
        force_ref[c] = total[c]
    speeds = [chunks(v8_ref[c]) for c in range(3)]

    def drifts(k, none):
        for c, speed in enumerate(lookup(speeds, list_ref[k])):
            drift_ref[k, c] = time_step * speed
        return none

    over_list(drifts, 0)


def md_kernel(arr_ref, p8_ref, v8_ref, force_ref, list_ref, near_in_ref, drift_in_ref,
              slot_ref, hot_ref, icnt_ref, f_ref,
              pos_ref, vel_ref, mom_ref, f_out_ref,
              near_ref, drift_ref, sem):
    saved = pltpu.make_async_copy(f_ref, f_out_ref, sem)
    saved.start()
    table = arr_ref[...].T
    slots = slot_ref[...]
    source = slots >> 2
    which = slots & 3
    target = []
    for c in range(4):
        value = lanes(spread(table, c), source)
        for r in range(1, 4):
            value = jnp.where(which == r, lanes(spread(table, r * 4 + c), source), value)
        target.append(value)
    drag = friction * target[3]
    pos = [p8_ref[c] for c in range(3)]
    vel = [v8_ref[c] for c in range(3)]
    here = list(pos)
    drift = [time_step * v for v in vel]
    for step in range(MD_STEPS):
        if step == 0:
            pair = [force_ref[c] for c in range(3)]
        else:
            from_near, from_drift = (
                (near_in_ref, drift_in_ref) if step == 1 else (near_ref, drift_ref)
            )
            miss = [pos[c] - (here[c] + drift[c]) for c in range(3)]
            largest = jnp.maximum(jnp.maximum(abs(miss[0]), abs(miss[1])), abs(miss[2]))
            largest = jnp.max(jnp.max(largest, axis=0, keepdims=True), axis=1, keepdims=True)
            largest = jnp.broadcast_to(jnp.maximum(largest, 1e-30), (8, 128))
            units = [largest * (1.0 / 1023.0), largest * (1.0 / 511.0)]
            rates = [1023.0 / largest, 511.0 / largest]
            pick = (0, 0, 1)
            whole_units = [
                jnp.floor(miss[c] * rates[pick[c]] + 0.5).astype(i32) for c in range(3)
            ]
            code = (
                (whole_units[0] << 21) | ((whole_units[1] & 2047) << 10) | (whole_units[2] & 1023)
            )
            for c in range(3):
                drift[c] = drift[c] + whole_units[c].astype(f32) * units[pick[c]]
                here[c] = here[c] + drift[c]
            tables = [chunks(code)]

            def entry(k, total):
                (word,) = lookup(tables, list_ref[k])
                words = (word >> 21, (word << 11) >> 21, (word << 22) >> 22)
                near = []
                for c in range(3):
                    move = from_drift[k, c] + words[c].astype(f32) * units[pick[c]]
                    drift_ref[k, c] = move
                    near.append(from_near[k, c] + move)
                    near_ref[k, c] = near[c]
                return pull(total, near, here)

            pair = over_list(entry, blank())
        for c in range(3):
            force = pair_strength * pair[c] + drag * (target[c] - vel[c])
            vel[c] = vel[c] + time_step * force
            pos[c] = pos[c] + time_step * vel[c]
    speed = vel[0] * vel[0] + vel[1] * vel[1] + vel[2] * vel[2]
    data = vel + [speed]
    row_id = lax.broadcasted_iota(i32, (16, 128), 0)
    comp = row_id & 3
    sums = jnp.zeros((128, 16), f32)
    for s in range(8):
        value = spread(data[0], s, 16)
        for c in range(1, 4):
            value = jnp.where(comp == c, spread(data[c], s, 16), value)
        value = jnp.where((spread(slots, s, 16) & 3) == (row_id >> 2), value, 0.0)
        hot = hot_ref[:, s * 128 : (s + 1) * 128]
        for part in range(3):
            piece = value.astype(bf16)
            value = value - piece.astype(f32)
            sums = sums + lax.dot_general(
                hot, piece, (((1,), (1,)), ((), ())), preferred_element_type=f32
            )
    mom_ref[...] = jnp.zeros((128, 128), f32)
    mom_ref[:, :16] = sums * icnt_ref[...]
    for c in range(3):
        for s in range(8):
            pos_ref[c : c + 1, s * 128 : (s + 1) * 128] = pos[c][s : s + 1, :]
            vel_ref[c : c + 1, s * 128 : (s + 1) * 128] = vel[c][s : s + 1, :]
    saved.wait()


def cell_kernel(back_ref, own_ref, rank_ref, out_ref):
    table = back_ref[...].T[:16, :]
    which = lax.broadcasted_iota(i32, (16, 128), 0) >> 2
    total = jnp.zeros((16, 128), f32)
    for k in range(2):
        picked = lanes(table, spread(own_ref[...], k, 16))
        total = total + jnp.where(spread(rank_ref[...], k, 16) == which, picked, 0.0)
    cell = total[0:4] + total[4:8] + total[8:12] + total[12:16]
    out_ref[:, 0, :] = cell[:, :64]
    out_ref[:, 1, :] = cell[:, 64:]


room = pltpu.CompilerParams(vmem_limit_bytes=16 << 20)


def shape(*dims, dtype=f32):
    return jax.ShapeDtypeStruct(dims, dtype)


def exchange(rows):
    return lax.all_to_all(rows, ("slab", "md"), split_axis=0, concat_axis=0, tiled=True)


near_pairs = [(i, i ^ 1) for i in range(32)]
far_pairs = [(i, (i + 1) % 32 if i % 2 else (i - 1) % 32) for i in range(32)]


def on_device(populations, relax, owners, positions, velocities, neighbours, atom_slots):
    slots = atom_slots.reshape(8, 128)
    eights = shape(3, 8, 128)
    own, inv, rank, hot, icnt, force, p8, v8, lists, near, drift = pl.pallas_call(
        prep_kernel,
        out_shape=(
            shape(8, 128, dtype=i32),
            shape(8, 128, dtype=i32),
            shape(8, 128, dtype=i32),
            shape(128, 1024, dtype=bf16),
            shape(128, 16),
            eights,
            eights,
            eights,
            shape(64, 8, 128, dtype=i32),
            shape(64, 3, 8, 128),
            shape(64, 3, 8, 128),
        ),
        name="prep", compiler_params=room,
    )(owners.transpose(0, 2, 1), slots, positions, velocities, neighbours.T)
    hbm = pl.BlockSpec(memory_space=pltpu.HBM)
    low, high, f_near, relax = pl.pallas_call(
        load_kernel,
        in_specs=[hbm, hbm],
        out_shape=(
            pltpu.VMEM((20, 2, 8, 128), f32),
            pltpu.VMEM((20, 2, 8, 128), f32),
            pltpu.VMEM((19, 2, 64, 128), f32),
            pltpu.VMEM((2, 64, 128), f32),
        ),
        scratch_shapes=[pltpu.SemaphoreType.DMA((9,))],
        name="load", compiler_params=room,
    )(
        pltpu.with_memory_space_constraint(populations, pltpu.HBM),
        pltpu.with_memory_space_constraint(relax, pltpu.HBM),
    )
    from_low = lax.ppermute(high, "md", [(i, (i + 1) % 4) for i in range(4)])
    from_high = lax.ppermute(low, "md", [((i + 1) % 4, i) for i in range(4)])
    post, up, down = pl.pallas_call(
        first_kernel,
        out_shape=(shape(19, 2, 64, 128), shape(20, 64, 128), shape(20, 64, 128)),
        name="first", compiler_params=room,
    )(f_near, relax)
    below = lax.ppermute(down, "slab", far_pairs)
    above = lax.ppermute(up, "slab", near_pairs)
    post_edge, up_edge, down_edge, relax_edge = pl.pallas_call(
        edge_kernel,
        out_shape=(
            shape(19, 2, 8, 128),
            shape(20, 8, 128),
            shape(20, 8, 128),
            shape(2, 8, 128),
        ),
        name="edge", compiler_params=room,
    )(from_low, from_high)
    below_edge = lax.ppermute(down_edge, "slab", far_pairs)
    above_edge = lax.ppermute(up_edge, "slab", near_pairs)
    scratch = [
        pltpu.VMEM((19, 2, PAD, 128), f32),
        pltpu.VMEM((5, PAD, 128), f32),
        pltpu.VMEM((5, PAD, 128), f32),
        pltpu.VMEM((len(sliding), 24, 128), f32),
        pltpu.VMEM((len(sliding), 24, 128), f32),
    ]
    post, up, down, relax_all = pl.pallas_call(
        middle_kernel,
        out_shape=(
            shape(19, 2, PAD, 128),
            shape(19, ROWS, 128),
            shape(19, ROWS, 128),
            shape(4, ROWS, 128),
        ),
        scratch_shapes=scratch + [pltpu.VMEM((2 * len(moving), 24, 128), f32)],
        name="middle", compiler_params=room,
    )(post, post_edge, below, above, below_edge, above_edge, relax, relax_edge)
    below = lax.ppermute(down, "slab", far_pairs)
    above = lax.ppermute(up, "slab", near_pairs)
    f, outgoing = pl.pallas_call(
        last_kernel,
        out_shape=(pltpu.VMEM((19, 2, 64, 128), f32), shape(128, 128)),
        scratch_shapes=scratch + [pltpu.VMEM((4, 128, 128), f32)],
        name="last", compiler_params=room,
    )(post, below, above, relax_all, inv)
    arrived = exchange(outgoing)
    vmem = pl.BlockSpec(memory_space=pltpu.VMEM)
    pos_out, vel_out, moms, f_out = pl.pallas_call(
        md_kernel,
        in_specs=[vmem] * 11,
        out_specs=(vmem, vmem, vmem, hbm),
        out_shape=(shape(3, 1024), shape(3, 1024), shape(128, 128), shape(19, 2, 64, 128)),
        scratch_shapes=[
            pltpu.VMEM((64, 3, 8, 128), f32),
            pltpu.VMEM((64, 3, 8, 128), f32),
            pltpu.SemaphoreType.DMA,
        ],
        name="md", compiler_params=room,
    )(arrived, p8, v8, force, lists, near, drift, slots, hot, icnt, f)
    returned = exchange(moms)
    cell = pl.pallas_call(cell_kernel, out_shape=shape(4, 2, 64), name="cells", compiler_params=room)(
        returned, own, rank
    )
    return (f_out, pos_out, vel_out, cell)


def solution(mesh):
    return jax.shard_map(
        on_device,
        mesh=mesh,
        in_specs=(
            P(None, "slab", "md", None),
            P("slab", "md", None),
            P("slab", "md", None),
            P(None, ("slab", "md")),
            P(None, ("slab", "md")),
            P(("slab", "md"), None),
            P(("slab", "md")),
        ),
        out_specs=(
            P(None, "slab", "md", None),
            P(None, ("slab", "md")),
            P(None, ("slab", "md")),
            P(None, "slab", "md"),
        ),
        check_vma=False,
    )
```

```python
import jax
import jax.numpy as jnp
from jax import lax
from jax.experimental import pallas as pl
from jax.experimental.pallas import tpu as pltpu
from jax.sharding import PartitionSpec as P

MD_STEPS = 5
f32 = jnp.float32
i32 = jnp.int32
bf16 = jnp.bfloat16

lattice_dirs = [
    (0, 0, 0),
    (1, 0, 0),
    (-1, 0, 0),
    (0, 1, 0),
    (0, -1, 0),
    (0, 0, 1),
    (0, 0, -1),
    (1, 1, 0),
    (-1, -1, 0),
    (1, -1, 0),
    (-1, 1, 0),
    (1, 0, 1),
    (-1, 0, -1),
    (1, 0, -1),
    (-1, 0, 1),
    (0, 1, 1),
    (0, -1, -1),
    (0, 1, -1),
    (0, -1, 1),
]
lattice_weights = [1.0 / 3.0] + [1.0 / 18.0] * 6 + [1.0 / 36.0] * 12
velocity_scale = 10.0
pair_strength = 0.5
friction = 2.0
time_step = 0.1


def mirrored(direction):
    return lattice_dirs.index((direction[0], direction[1], -direction[2]))


flip = [mirrored(c) for c in lattice_dirs]
rising = [i for i, c in enumerate(lattice_dirs) if c[2] == 1]
falling = [flip[i] for i in rising]
level = [i for i, c in enumerate(lattice_dirs) if c[2] == 0]
pairs = [(1, 2), (3, 4), (5, 6)] + [(i, i + 1) for i in range(7, 19, 2)]
SENT = 13
ROWS = 72
PAD = 88


def parity():
    return lax.axis_index("slab") & 1


def actual(index, odd):
    return jnp.where(odd == 1, flip[index], index)


def moments_of(f):
    s = {}
    for plus, minus in pairs:
        s[plus] = (f[plus] + f[minus], f[plus] - f[minus])
    density = f[0]
    for plus, _ in pairs:
        density = density + s[plus][0]
    flow = []
    for axis_id in range(3):
        total = None
        for plus, _ in pairs:
            sign = lattice_dirs[plus][axis_id]
            if sign == 0:
                continue
            term = s[plus][1]
            if total is None:
                total = term
            else:
                total = total + term if sign > 0 else total - term
        flow.append(total)
    return density, flow


def collided(f, relax, wanted):
    density, flow = moments_of(f)
    inverse = 1.0 / density
    vel = [j * inverse for j in flow]
    usq = vel[0] * vel[0] + vel[1] * vel[1] + vel[2] * vel[2]
    keep = 1.0 - relax
    gain = relax * density
    base = gain - (1.5 * gain) * usq
    result = {}
    if 0 in wanted:
        result[0] = keep * f[0] + lattice_weights[0] * base
    for plus, minus in pairs:
        if plus not in wanted and minus not in wanted:
            continue
        along = None
        for axis_id in range(3):
            sign = lattice_dirs[plus][axis_id]
            if sign != 0:
                part = vel[axis_id]
                if along is None:
                    along = part
                else:
                    along = along + part if sign > 0 else along - part
        weight = lattice_weights[plus]
        slope = (3.0 * weight) * (gain * along)
        even = weight * base + 1.5 * (along * slope)
        if plus in wanted:
            result[plus] = keep * f[plus] + (even + slope)
        if minus in wanted:
            result[minus] = keep * f[minus] + (even - slope)
    return {i: rolled(v, lattice_dirs[i][1]) for i, v in result.items()}


def rolled(block, by):
    return block if by == 0 else pltpu.roll(block, by % 128, 1)


def put(ref, where, block_id, value):
    ref[(*where, pl.ds(8 + 8 * block_id, 8), slice(None))] = value
    if block_id == 0:
        ref[(*where, pl.ds(8 + ROWS, 1), slice(None))] = value[0:1, :]
    if block_id == 8:
        ref[(*where, pl.ds(7, 1), slice(None))] = value[7:8, :]


def get(ref, where, block_id, shift):
    return ref[(*where, pl.ds(8 + 8 * block_id - shift, 8), slice(None))]


def rows_of(block_id):
    return pl.ds(8 * block_id, 8)


def outgoing_planes(store, read, near, far, ways, relax):
    for k, i in enumerate(ways):
        store(k, read(i, near))
        store(5 + k, read(i, far))
    flat = {i: read(i, near) for i in level}
    sums = [None, None, None]
    for i, value in flat.items():
        for n, sign in enumerate((1,) + lattice_dirs[i][:2]):
            if sign == 0:
                continue
            if sums[n] is None:
                sums[n] = value if sign > 0 else -value
            else:
                sums[n] = sums[n] + value if sign > 0 else sums[n] - value
    for n in range(3):
        store(10 + n, sums[n])
    if relax is not None:
        store(SENT, relax)


def storing(out_ref, b):
    def store(j, value):
        out_ref[j, rows_of(b), :] = value

    return store


def halo_collided(from_halo, from_own, sums, relax, ways, back):
    density, flow_x, flow_y = sums
    arriving = None
    leaving = None
    for k in range(5):
        x, y, _ = lattice_dirs[ways[k]]
        density = density + (from_halo[k] + from_own[k])
        arriving = from_halo[k] if arriving is None else arriving + from_halo[k]
        leaving = from_own[k] if leaving is None else leaving + from_own[k]
        back_x, back_y, _ = lattice_dirs[back[k]]
        for sign, value in ((x, from_halo[k]), (back_x, from_own[k])):
            if sign != 0:
                flow_x = flow_x + value if sign > 0 else flow_x - value
        for sign, value in ((y, from_halo[k]), (back_y, from_own[k])):
            if sign != 0:
                flow_y = flow_y + value if sign > 0 else flow_y - value
    inverse = 1.0 / density
    vel_x = flow_x * inverse
    vel_y = flow_y * inverse
    towards = (arriving - leaving) * inverse
    usq = vel_x * vel_x + vel_y * vel_y + towards * towards
    keep = 1.0 - relax
    gain = relax * density
    base = gain - (1.5 * gain) * usq
    result = []
    for k in range(5):
        x, y, _ = lattice_dirs[ways[k]]
        along = towards
        if x != 0:
            along = along + vel_x if x > 0 else along - vel_x
        if y != 0:
            along = along + vel_y if y > 0 else along - vel_y
        weight = lattice_weights[ways[k]]
        slope = (3.0 * weight) * (gain * along)
        equil = weight * base + (slope + 1.5 * (along * slope))
        result.append(rolled(keep * from_halo[k] + equil, y))
    return result


everything = set(range(19))


def first_kernel(f_hbm_ref, relax_hbm_ref,
                 low_ref, high_ref, relax_ref, post_ref, up_ref, down_ref,
                 f_ref, pad_ref, sems):
    odd = parity()
    copies = [pltpu.make_async_copy(relax_hbm_ref, relax_ref, sems.at[4])]
    quarters = [(plane, half) for plane in range(2) for half in range(2)]
    for n, (plane, half) in enumerate(quarters):
        part = (slice(None), plane, pl.ds(32 * half, 32), slice(None))
        copies.append(pltpu.make_async_copy(f_hbm_ref.at[part], f_ref.at[part], sems.at[n]))
    for copy in copies:
        copy.start()
    copies[0].wait()
    for n, (actual_plane, half) in enumerate(quarters):
        copies[1 + n].wait()
        plane = jnp.where(odd == 1, 1 - actual_plane, actual_plane)
        for b in range(4 * half, 4 * half + 4):
            f = {i: f_ref[actual(i, odd), actual_plane, rows_of(b), :] for i in range(19)}
            post = collided(f, relax_ref[actual_plane, rows_of(b), :], everything)
            for i in range(19):
                post_ref[i, plane, rows_of(b), :] = post[i]
                if lattice_dirs[i][0] != 0:
                    pad_ref[i, plane, pl.ds(8 + 8 * b, 8), :] = post[i]
    head = lax.broadcasted_iota(i32, (8, 128), 0) < 4
    for i in range(20):
        ends = [
            [
                (f_ref[i, plane, rows_of(b), :] if i < 19 else relax_ref[plane, rows_of(b), :])
                for plane in range(2)
            ]
            for b in (0, 7)
        ]
        low_ref[i] = jnp.where(head, ends[0][0], pltpu.roll(ends[0][1], 4, 0))
        high_ref[i] = jnp.where(head, pltpu.roll(ends[1][0], 4, 0), ends[1][1])
    for plane in range(2):
        actual_plane = jnp.where(odd == 1, 1 - plane, plane)
        out_ref, ways = (up_ref, rising) if plane == 1 else (down_ref, falling)
        for b in range(8):

            def read(i, source):
                shift = lattice_dirs[i][0]
                if shift == 0:
                    return post_ref[i, source, rows_of(b), :]
                return pad_ref[i, source, pl.ds(8 + 8 * b - shift, 8), :]

            outgoing_planes(
                storing(out_ref, b), read, plane, 1 - plane, ways,
                relax_ref[actual_plane, rows_of(b), :],
            )


def edge_kernel(low_ref, high_ref, post_ref, seam_ref, up_ref, down_ref, relax_ref):
    odd = parity()
    row_id = lax.broadcasted_iota(i32, (8, 128), 0)
    mixed_relax = []
    for plane in range(2):
        actual_plane = jnp.where(odd == 1, 1 - plane, plane)
        upper = jnp.broadcast_to(actual_plane, (8, 128)) == 1
        mixed = []
        for i in range(20):
            j = actual(i, odd) if i < 19 else i
            high = high_ref[j]
            low = low_ref[j]
            high = jnp.where(upper, pltpu.roll(high, 4, 0), high)
            low = jnp.where(upper, low, pltpu.roll(low, 4, 0))
            mixed.append(jnp.where(row_id < 4, high, low))
        post = collided(dict(enumerate(mixed[:19])), mixed[19], everything)
        relax_ref[plane] = mixed[19]
        mixed_relax.append(mixed[19])
        for i in range(19):
            seam_ref[2 * i + plane, 0:8, :] = post_ref[i, plane, 56:64, :]
            seam_ref[2 * i + plane, 8:16, :] = post[i]
            seam_ref[2 * i + plane, 16:24, :] = post_ref[i, plane, 0:8, :]

    def read(i, source):
        shift = lattice_dirs[i][0]
        at = [seam_ref[2 * i + source, pl.ds(start - shift, 8), :] for start in (4, 8, 12)]
        return jnp.where(row_id == 3, at[0], jnp.where(row_id == 4, at[2], at[1]))

    outgoing_planes(storing(up_ref, 0), read, 1, 0, rising, mixed_relax[1])
    outgoing_planes(storing(down_ref, 0), read, 0, 1, falling, mixed_relax[0])


def two_steps(own, below, above, relax, second_ref, from_below_ref, from_above_ref):
    for b in range(9):
        for plane in range(2):
            f = {}
            for i, c in enumerate(lattice_dirs):
                source = plane - c[2]
                if source in (0, 1):
                    f[i] = own(i, source, b, c[0])
                elif source < 0:
                    f[i] = below(rising.index(i), b)
                else:
                    f[i] = above(falling.index(i), b)
            post = collided(f, relax(plane, b), everything)
            for i, value in post.items():
                put(second_ref, (i, plane), b, value)
        for side, ways, back, source, plane, out_ref in (
            (below, rising, falling, 0, -1, from_below_ref),
            (above, falling, rising, 1, 2, from_above_ref),
        ):
            post = halo_collided(
                [side(5 + k, b) for k in range(5)],
                [own(i, source, b, lattice_dirs[i][0]) for i in back],
                [side(10 + n, b) for n in range(3)],
                relax(plane, b), ways, back,
            )
            for k in range(5):
                put(out_ref, (k,), b, post[k])


def streamed(second_ref, from_below_ref, from_above_ref, plane, b):
    f = {}
    for i, c in enumerate(lattice_dirs):
        source = plane - c[2]
        if source == -1:
            f[i] = get(from_below_ref, (rising.index(i),), b, c[0])
        elif source == 2:
            f[i] = get(from_above_ref, (falling.index(i),), b, c[0])
        else:
            f[i] = get(second_ref, (i, source), b, c[0])
    return f


def middle_kernel(post_ref, seam_ref, below_ref, above_ref, below_edge_ref, above_edge_ref,
                  relax_ref, relax_edge_ref,
                  third_ref, up_ref, down_ref, relax_out_ref,
                  second_ref, from_below_ref, from_above_ref):
    odd = parity()
    row_id = lax.broadcasted_iota(i32, (8, 128), 0)

    def own(i, plane, b, shift):
        if b == 8:
            return seam_ref[2 * i + plane, 8 - shift : 16 - shift, :]
        if b == 0 and shift == 1:
            return seam_ref[2 * i + plane, 15:23, :]
        if b == 7 and shift == -1:
            return seam_ref[2 * i + plane, 1:9, :]
        return post_ref[i, plane, 8 * b - shift : 8 * b - shift + 8, :]

    def joined(main_ref, edge_ref):
        def read(j, b):
            if b == 8:
                return edge_ref[j]
            if b in (0, 7):
                turned = pltpu.roll(edge_ref[j], 4, 0)
                return jnp.where(row_id == b, turned, main_ref[j, rows_of(b), :])
            return main_ref[j, rows_of(b), :]

        return read

    below = joined(below_ref, below_edge_ref)
    above = joined(above_ref, above_edge_ref)
    for b in range(8):
        relax_out_ref[0, rows_of(b), :] = below_ref[SENT, rows_of(b), :]
        relax_out_ref[3, rows_of(b), :] = above_ref[SENT, rows_of(b), :]
        for plane in range(2):
            relax_out_ref[1 + plane, rows_of(b), :] = relax_ref[
                jnp.where(odd == 1, 1 - plane, plane), rows_of(b), :
            ]
    relax_out_ref[0, rows_of(8), :] = below_edge_ref[SENT]
    relax_out_ref[3, rows_of(8), :] = above_edge_ref[SENT]
    for plane in range(2):
        relax_out_ref[1 + plane, rows_of(8), :] = relax_edge_ref[plane]

    def relax(plane, b):
        return relax_out_ref[1 + plane, rows_of(b), :]

    two_steps(own, below, above, relax, second_ref, from_below_ref, from_above_ref)
    for b in range(9):
        for plane in range(2):
            f = streamed(second_ref, from_below_ref, from_above_ref, plane, b)
            post = collided(f, relax(plane, b), everything)
            for i in range(19):
                put(third_ref, (i, plane), b, post[i])
    for b in range(9):

        def read(i, source):
            return get(third_ref, (i, source), b, lattice_dirs[i][0])

        for out_ref, near, ways in ((up_ref, 1, rising), (down_ref, 0, falling)):
            ends = {}

            def store(j, value):
                if b < 8:
                    out_ref[8 * j + b] = value
                else:
                    ends[j] = pltpu.roll(value, 2 * (j % 4) + 1, 0)

            outgoing_planes(store, read, near, 1 - near, ways, None)
            for group in range(4 if ends else 0):
                block = ends[4 * group]
                for m in range(1, min(4, SENT - 4 * group)):
                    block = jnp.where((row_id >> 1) == m, ends[4 * group + m], block)
                out_ref[8 * SENT + group] = block


def last_kernel(post_ref, below_ref, above_ref, relax_ref, inv_ref,
                f_ref, out_ref,
                second_ref, from_below_ref, from_above_ref, flow_ref):
    odd = parity()

    def side(ref):
        def read(j, b):
            if b < 8:
                return ref[8 * j + b]
            return pltpu.roll(ref[8 * SENT + j // 4], 7 - 2 * (j % 4), 0)

        return read

    below = side(below_ref)
    above = side(above_ref)

    def own(i, plane, b, shift):
        return get(post_ref, (i, plane), b, shift)

    def relax(plane, b):
        return relax_ref[1 + plane, rows_of(b), :]

    two_steps(own, below, above, relax, second_ref, from_below_ref, from_above_ref)
    upward = jnp.where(odd == 1, -velocity_scale / 128.0, velocity_scale / 128.0)
    for plane in range(2):
        actual_plane = jnp.where(odd == 1, 1 - plane, plane)
        for b in range(8):
            f = streamed(second_ref, from_below_ref, from_above_ref, plane, b)
            for i in range(19):
                f_ref[actual(i, odd), actual_plane, rows_of(b), :] = f[i]
            density, flow = moments_of(f)
            inverse = 1.0 / density
            where = pl.ds(pl.multiple_of(actual_plane * 64 + 8 * b, 8), 8)
            flow_ref[0, where, :] = flow[0] * inverse * (velocity_scale / 128.0)
            flow_ref[1, where, :] = flow[1] * inverse * (velocity_scale / 128.0)
            flow_ref[2, where, :] = flow[2] * inverse * upward
            flow_ref[3, where, :] = density * (1.0 / 128.0)
    means = [jnp.sum(flow_ref[c].T, axis=0, keepdims=True) for c in range(4)]
    packed = jnp.concatenate(means * 4, axis=0)
    inv16 = jnp.concatenate(
        [jnp.broadcast_to(inv_ref[r : r + 1, :], (4, 128)) for r in range(4)], axis=0
    )
    picked = jnp.where(inv16 >= 0, lanes(packed, jnp.maximum(inv16, 0)), 0.0)
    out_ref[...] = jnp.concatenate([picked, jnp.zeros((112, 128), f32)], axis=0).T


def lanes(table, index):
    return jnp.take_along_axis(table, index, axis=1, mode="promise_in_bounds")


def spread(block, index, rows=8):
    return jnp.broadcast_to(block[index : index + 1, :], (rows, 128))


def lookup(tables, index):
    low = index & 127
    found = [[lanes(chunk, low) for chunk in table] for table in tables]
    for mask in (128, 256, 512):
        bit = (index & mask) != 0
        found = [
            [jnp.where(bit, f[2 * j + 1], f[2 * j]) for j in range(len(f) // 2)] for f in found
        ]
    return [f[0] for f in found]


def chunks(block):
    return [spread(block, chunk) for chunk in range(8)]


def pull(total, near, here):
    gaps = [n - h for n, h in zip(near, here)]
    weight = jnp.exp(-0.5 * (gaps[0] * gaps[0] + gaps[1] * gaps[1] + gaps[2] * gaps[2]))
    return tuple(t + g * weight for t, g in zip(total, gaps))


def over_list(entry, start, unroll):
    return lax.fori_loop(0, 64, entry, start, unroll=unroll)


def blank():
    return tuple(jnp.zeros((8, 128), f32) for _ in range(3))


def prep_kernel(own_in_ref, slot_ref, pos_ref, vel_ref, nbr_ref,
                own_ref, inv_ref, rank_ref, hot_ref, icnt_ref, force_ref, p8_ref, v8_ref,
                list_ref, near_ref, drift_ref):
    for k in range(2):
        for z in range(2):
            own_ref[k : k + 1, z * 64 : (z + 1) * 64] = own_in_ref[z, k : k + 1, :]
    own_ref[2:8, :] = jnp.zeros((6, 128), i32)
    row_id = lax.broadcasted_iota(i32, (128, 128), 0)
    lane_id = lax.broadcasted_iota(i32, (128, 128), 1)
    own = [spread(own_ref[...], k, 128) for k in range(2)]
    own_t = [o.T for o in own]
    ranks = []
    for k in range(2):
        count = jnp.zeros((128, 128), i32)
        for other in range(2):
            count = count + jnp.where((own_t[other] == own[k]) & (row_id < lane_id), 1, 0)
        ranks.append(jnp.sum(count, axis=0, keepdims=True))
    rank_ref[...] = jnp.concatenate(ranks + [jnp.zeros((6, 128), i32)], axis=0)
    rank_t = [jnp.broadcast_to(r, (128, 128)).T for r in ranks]
    rows = []
    for r in range(4):
        cell = jnp.zeros((128, 128), i32)
        for k in range(2):
            cell = cell + jnp.where((own_t[k] == lane_id) & (rank_t[k] == r), row_id + 1, 0)
        rows.append(jnp.sum(cell, axis=0, keepdims=True) - 1)
    inv_ref[...] = jnp.concatenate(rows + [jnp.zeros((4, 128), i32)], axis=0)
    slots = slot_ref[...]
    count = jnp.zeros((128, 16), f32)
    want = lax.broadcasted_iota(i32, (16, 128), 0) >> 2
    for s in range(8):
        one = spread(slots, s, 128)
        hot = jnp.where((one >> 2) == row_id, 1.0, 0.0).astype(bf16)
        hot_ref[:, s * 128 : (s + 1) * 128] = hot
        match = jnp.where((spread(slots, s, 16) & 3) == want, 1.0, 0.0).astype(bf16)
        count = count + lax.dot_general(
            hot, match, (((1,), (1,)), ((), ())), preferred_element_type=f32
        )
    icnt_ref[...] = 1.0 / jnp.maximum(count, 1.0)
    for c in range(3):
        for s in range(8):
            p8_ref[c, s : s + 1, :] = pos_ref[c : c + 1, s * 128 : (s + 1) * 128]
            v8_ref[c, s : s + 1, :] = vel_ref[c : c + 1, s * 128 : (s + 1) * 128]
    for k in range(8):
        for part in range(8):
            list_ref[8 * k : 8 * k + 8, part, :] = nbr_ref[
                8 * k : 8 * k + 8, part * 128 : (part + 1) * 128
            ]
    here = [p8_ref[c] for c in range(3)]
    tables = [chunks(h) for h in here]

    def positions(k, total):
        near = lookup(tables, list_ref[k])
        for c in range(3):
            near_ref[k, c] = near[c]
        return pull(total, near, here)

    total = over_list(positions, blank(), 32)
    for c in range(3):
        force_ref[c] = total[c]
    speeds = [chunks(v8_ref[c]) for c in range(3)]

    def drifts(k, none):
        for c, speed in enumerate(lookup(speeds, list_ref[k])):
            drift_ref[k, c] = time_step * speed
        return none

    over_list(drifts, 0, 32)


def md_kernel(arr_ref, p8_ref, v8_ref, force_ref, list_ref, near_in_ref, drift_in_ref,
              slot_ref, hot_ref, icnt_ref, f_ref,
              pos_out_ref, vel_out_ref, mom_ref, f_out_ref,
              near_ref, drift_ref, pos_ref, vel_ref, sems):
    saved = [
        pltpu.make_async_copy(f_ref, f_out_ref, sems.at[0]),
        pltpu.make_async_copy(pos_ref, pos_out_ref, sems.at[1]),
        pltpu.make_async_copy(vel_ref, vel_out_ref, sems.at[2]),
    ]
    saved[0].start()
    table = arr_ref[...].T
    slots = slot_ref[...]
    source = slots >> 2
    which = slots & 3
    target = []
    for c in range(4):
        value = lanes(spread(table, c), source)
        for r in range(1, 4):
            value = jnp.where(which == r, lanes(spread(table, r * 4 + c), source), value)
        target.append(value)
    drag = friction * target[3]
    pos = [p8_ref[c] for c in range(3)]
    vel = [v8_ref[c] for c in range(3)]
    here = list(pos)
    drift = [time_step * v for v in vel]
    for step in range(MD_STEPS):
        if step == 0:
            pair = [force_ref[c] for c in range(3)]
        else:
            from_near, from_drift = (
                (near_in_ref, drift_in_ref) if step == 1 else (near_ref, drift_ref)
            )
            miss = [pos[c] - (here[c] + drift[c]) for c in range(3)]
            largest = jnp.maximum(jnp.maximum(abs(miss[0]), abs(miss[1])), abs(miss[2]))
            largest = jnp.max(jnp.max(largest, axis=0, keepdims=True), axis=1, keepdims=True)
            largest = jnp.broadcast_to(jnp.maximum(largest, 1e-30), (8, 128))
            units = [largest * (1.0 / 1023.0), largest * (1.0 / 511.0)]
            rates = [1023.0 / largest, 511.0 / largest]
            pick = (0, 0, 1)
            whole_units = [
                jnp.floor(miss[c] * rates[pick[c]] + 0.5).astype(i32) for c in range(3)
            ]
            code = (
                (whole_units[0] << 21) | ((whole_units[1] & 2047) << 10) | (whole_units[2] & 1023)
            )
            for c in range(3):
                drift[c] = drift[c] + whole_units[c].astype(f32) * units[pick[c]]
                here[c] = here[c] + drift[c]
            tables = [chunks(code)]

            def entry(k, total):
                (word,) = lookup(tables, list_ref[k])
                words = (word >> 21, (word << 11) >> 21, (word << 22) >> 22)
                near = []
                for c in range(3):
                    move = from_drift[k, c] + words[c].astype(f32) * units[pick[c]]
                    drift_ref[k, c] = move
                    near.append(from_near[k, c] + move)
                    near_ref[k, c] = near[c]
                return pull(total, near, here)

            pair = over_list(entry, blank(), 64)
        for c in range(3):
            force = pair_strength * pair[c] + drag * (target[c] - vel[c])
            vel[c] = vel[c] + time_step * force
            pos[c] = pos[c] + time_step * vel[c]
    for c in range(3):
        for s in range(8):
            pos_ref[c : c + 1, s * 128 : (s + 1) * 128] = pos[c][s : s + 1, :]
            vel_ref[c : c + 1, s * 128 : (s + 1) * 128] = vel[c][s : s + 1, :]
    saved[1].start()
    saved[2].start()
    speed = vel[0] * vel[0] + vel[1] * vel[1] + vel[2] * vel[2]
    data = vel + [speed]
    row_id = lax.broadcasted_iota(i32, (16, 128), 0)
    comp = row_id & 3
    sums = jnp.zeros((128, 16), f32)
    for s in range(8):
        value = spread(data[0], s, 16)
        for c in range(1, 4):
            value = jnp.where(comp == c, spread(data[c], s, 16), value)
        value = jnp.where((spread(slots, s, 16) & 3) == (row_id >> 2), value, 0.0)
        hot = hot_ref[:, s * 128 : (s + 1) * 128]
        for _ in range(3):
            piece = value.astype(bf16)
            value = value - piece.astype(f32)
            sums = sums + lax.dot_general(
                hot, piece, (((1,), (1,)), ((), ())), preferred_element_type=f32
            )
    mom_ref[...] = jnp.zeros((128, 128), f32)
    mom_ref[:, :16] = sums * icnt_ref[...]
    for copy in saved:
        copy.wait()


def cell_kernel(back_ref, own_ref, rank_ref, out_ref):
    table = back_ref[...].T[:16, :]
    which = lax.broadcasted_iota(i32, (16, 128), 0) >> 2
    total = jnp.zeros((16, 128), f32)
    for k in range(2):
        picked = lanes(table, spread(own_ref[...], k, 16))
        total = total + jnp.where(spread(rank_ref[...], k, 16) == which, picked, 0.0)
    cell = total[0:4] + total[4:8] + total[8:12] + total[12:16]
    out_ref[:, 0, :] = cell[:, :64]
    out_ref[:, 1, :] = cell[:, 64:]


room = pltpu.CompilerParams(vmem_limit_bytes=16 << 20)


def shape(*dims, dtype=f32):
    return jax.ShapeDtypeStruct(dims, dtype)


def exchange(rows):
    return lax.all_to_all(rows, ("slab", "md"), split_axis=0, concat_axis=0, tiled=True)


near_pairs = [(i, i ^ 1) for i in range(32)]
far_pairs = [(i, (i + 1) % 32 if i % 2 else (i - 1) % 32) for i in range(32)]


def whole(populations, relax, owners, positions, velocities, neighbours, atom_slots):
    slots = atom_slots.reshape(8, 128)
    eights = shape(3, 8, 128)
    own, inv, rank, hot, icnt, force, p8, v8, lists, near, drift = pl.pallas_call(
        prep_kernel,
        out_shape=(
            shape(8, 128, dtype=i32),
            shape(8, 128, dtype=i32),
            shape(8, 128, dtype=i32),
            shape(128, 1024, dtype=bf16),
            shape(128, 16),
            eights,
            eights,
            eights,
            shape(64, 8, 128, dtype=i32),
            shape(64, 3, 8, 128),
            shape(64, 3, 8, 128),
        ),
        name="prep", compiler_params=room,
    )(owners.transpose(0, 2, 1), slots, positions, velocities, neighbours.T)
    hbm = pl.BlockSpec(memory_space=pltpu.HBM)
    low, high, relax, post, up, down = pl.pallas_call(
        first_kernel,
        in_specs=[hbm, hbm],
        out_shape=(
            pltpu.VMEM((20, 8, 128), f32),
            pltpu.VMEM((20, 8, 128), f32),
            pltpu.VMEM((2, 64, 128), f32),
            pltpu.VMEM((19, 2, 64, 128), f32),
            pltpu.VMEM((SENT + 1, 64, 128), f32),
            pltpu.VMEM((SENT + 1, 64, 128), f32),
        ),
        scratch_shapes=[
            pltpu.VMEM((19, 2, 64, 128), f32),
            pltpu.VMEM((19, 2, 80, 128), f32),
            pltpu.SemaphoreType.DMA((5,)),
        ],
        name="first", compiler_params=room,
    )(
        pltpu.with_memory_space_constraint(populations, pltpu.HBM),
        pltpu.with_memory_space_constraint(relax, pltpu.HBM),
    )
    below = lax.ppermute(down, "slab", far_pairs)
    from_low = lax.ppermute(high, "md", [(i, (i + 1) % 4) for i in range(4)])
    from_high = lax.ppermute(low, "md", [((i + 1) % 4, i) for i in range(4)])
    above = lax.ppermute(up, "slab", near_pairs)
    seam, up_edge, down_edge, relax_edge = pl.pallas_call(
        edge_kernel,
        out_shape=(
            shape(38, 24, 128),
            shape(SENT + 1, 8, 128),
            shape(SENT + 1, 8, 128),
            shape(2, 8, 128),
        ),
        name="edge", compiler_params=room,
    )(from_low, from_high, post)
    below_edge = lax.ppermute(down_edge, "slab", far_pairs)
    above_edge = lax.ppermute(up_edge, "slab", near_pairs)
    scratch = [
        pltpu.VMEM((19, 2, PAD, 128), f32),
        pltpu.VMEM((5, PAD, 128), f32),
        pltpu.VMEM((5, PAD, 128), f32),
    ]
    post, up, down, relax_all = pl.pallas_call(
        middle_kernel,
        out_shape=(
            shape(19, 2, PAD, 128),
            shape(8 * SENT + 4, 8, 128),
            shape(8 * SENT + 4, 8, 128),
            shape(4, ROWS, 128),
        ),
        scratch_shapes=scratch,
        name="middle", compiler_params=room,
    )(post, seam, below, above, below_edge, above_edge, relax, relax_edge)
    below = lax.ppermute(down, "slab", far_pairs)
    above = lax.ppermute(up, "slab", near_pairs)
    f, outgoing = pl.pallas_call(
        last_kernel,
        out_shape=(pltpu.VMEM((19, 2, 64, 128), f32), shape(128, 128)),
        scratch_shapes=scratch + [pltpu.VMEM((4, 128, 128), f32)],
        name="last", compiler_params=room,
    )(post, below, above, relax_all, inv)
    arrived = exchange(outgoing)
    vmem = pl.BlockSpec(memory_space=pltpu.VMEM)
    pos_out, vel_out, moms, f_out = pl.pallas_call(
        md_kernel,
        in_specs=[vmem] * 11,
        out_specs=(hbm, hbm, vmem, hbm),
        out_shape=(
            shape(3, 1024), shape(3, 1024), shape(128, 128), shape(19, 2, 64, 128)
        ),
        scratch_shapes=[
            pltpu.VMEM((64, 3, 8, 128), f32),
            pltpu.VMEM((64, 3, 8, 128), f32),
            pltpu.VMEM((3, 1024), f32),
            pltpu.VMEM((3, 1024), f32),
            pltpu.SemaphoreType.DMA((3,)),
        ],
        name="md", compiler_params=room,
    )(arrived, p8, v8, force, lists, near, drift, slots, hot, icnt, f)
    returned = exchange(moms)
    cell = pl.pallas_call(
        cell_kernel, out_shape=shape(4, 2, 64), name="cells", compiler_params=room
    )(returned, own, rank)
    return (f_out, pos_out, vel_out, cell)


def solution(mesh):
    return jax.shard_map(
        whole,
        mesh=mesh,
        in_specs=(
            P(None, "slab", "md", None),
            P("slab", "md", None),
            P("slab", "md", None),
            P(None, ("slab", "md")),
            P(None, ("slab", "md")),
            P(("slab", "md"), None),
            P(("slab", "md")),
        ),
        out_specs=(
            P(None, "slab", "md", None),
            P(None, ("slab", "md")),
            P(None, ("slab", "md")),
            P(None, "slab", "md"),
        ),
        check_vma=False,
    )
```

```python
import math

import jax
import jax.numpy as jnp
from jax import lax
from jax.experimental import pallas as pl
from jax.experimental.pallas import tpu as pltpu
from jax.sharding import PartitionSpec as P

MD_STEPS = 5
f32 = jnp.float32
i32 = jnp.int32
bf16 = jnp.bfloat16

lattice_dirs = [
    (0, 0, 0),
    (1, 0, 0),
    (-1, 0, 0),
    (0, 1, 0),
    (0, -1, 0),
    (0, 0, 1),
    (0, 0, -1),
    (1, 1, 0),
    (-1, -1, 0),
    (1, -1, 0),
    (-1, 1, 0),
    (1, 0, 1),
    (-1, 0, -1),
    (1, 0, -1),
    (-1, 0, 1),
    (0, 1, 1),
    (0, -1, -1),
    (0, 1, -1),
    (0, -1, 1),
]
lattice_weights = [1.0 / 3.0] + [1.0 / 18.0] * 6 + [1.0 / 36.0] * 12
velocity_scale = 10.0
pair_strength = 0.5
friction = 2.0
time_step = 0.1


def mirrored(direction):
    return lattice_dirs.index((direction[0], direction[1], -direction[2]))


flip = [mirrored(c) for c in lattice_dirs]
rising = [i for i, c in enumerate(lattice_dirs) if c[2] == 1]
falling = [flip[i] for i in rising]
level = [i for i, c in enumerate(lattice_dirs) if c[2] == 0]
pairs = [(1, 2), (3, 4), (5, 6)] + [(i, i + 1) for i in range(7, 19, 2)]
SENT = 13
ROWS = 72
PAD = 88


def parity():
    return lax.axis_index("slab") & 1


def actual(index, odd):
    return jnp.where(odd == 1, flip[index], index)


def moments_of(f):
    s = {}
    for plus, minus in pairs:
        s[plus] = (f[plus] + f[minus], f[plus] - f[minus])
    density = f[0]
    for plus, _ in pairs:
        density = density + s[plus][0]
    flow = []
    for axis_id in range(3):
        total = None
        for plus, _ in pairs:
            sign = lattice_dirs[plus][axis_id]
            if sign == 0:
                continue
            term = s[plus][1]
            if total is None:
                total = term
            else:
                total = total + term if sign > 0 else total - term
        flow.append(total)
    return density, flow


def collided(f, relax, wanted):
    density, flow = moments_of(f)
    inverse = 1.0 / density
    vel = [j * inverse for j in flow]
    usq = vel[0] * vel[0] + vel[1] * vel[1] + vel[2] * vel[2]
    keep = 1.0 - relax
    gain = relax * density
    base = gain - (1.5 * gain) * usq
    scaled = {w: (w * base, (3.0 * w) * gain, (4.5 * w) * gain) for w in lattice_weights[1::6]}
    result = {}
    if 0 in wanted:
        result[0] = keep * f[0] + lattice_weights[0] * base
    for plus, minus in pairs:
        if plus not in wanted and minus not in wanted:
            continue
        along = None
        for axis_id in range(3):
            sign = lattice_dirs[plus][axis_id]
            if sign != 0:
                part = vel[axis_id]
                if along is None:
                    along = part
                else:
                    along = along + part if sign > 0 else along - part
        still, linear, square = scaled[lattice_weights[plus]]
        slope = linear * along
        even = still + (square * along) * along
        if plus in wanted:
            result[plus] = keep * f[plus] + (even + slope)
        if minus in wanted:
            result[minus] = keep * f[minus] + (even - slope)
    return {i: rolled(v, lattice_dirs[i][1]) for i, v in result.items()}


def rolled(block, by):
    return block if by == 0 else pltpu.roll(block, by % 128, 1)


def put(ref, where, block_id, value):
    ref[(*where, pl.ds(8 + 8 * block_id, 8), slice(None))] = value
    if block_id == 0:
        ref[(*where, pl.ds(8 + ROWS, 1), slice(None))] = value[0:1, :]
    if block_id == 8:
        ref[(*where, pl.ds(7, 1), slice(None))] = value[7:8, :]


def get(ref, where, block_id, shift):
    return ref[(*where, pl.ds(8 + 8 * block_id - shift, 8), slice(None))]


def rows_of(block_id):
    return pl.ds(8 * block_id, 8)


def outgoing_planes(store, read, near, far, ways, relax):
    for k, i in enumerate(ways):
        store(k, read(i, near))
        store(5 + k, read(i, far))
    flat = {i: read(i, near) for i in level}
    sums = [None, None, None]
    for i, value in flat.items():
        for n, sign in enumerate((1,) + lattice_dirs[i][:2]):
            if sign == 0:
                continue
            if sums[n] is None:
                sums[n] = value if sign > 0 else -value
            else:
                sums[n] = sums[n] + value if sign > 0 else sums[n] - value
    for n in range(3):
        store(10 + n, sums[n])
    if relax is not None:
        store(SENT, relax)


def storing(out_ref, b):
    def store(j, value):
        out_ref[j, rows_of(b), :] = value

    return store


def halo_collided(from_halo, from_own, sums, relax, ways, back):
    density, flow_x, flow_y = sums
    arriving = None
    leaving = None
    for k in range(5):
        x, y, _ = lattice_dirs[ways[k]]
        density = density + (from_halo[k] + from_own[k])
        arriving = from_halo[k] if arriving is None else arriving + from_halo[k]
        leaving = from_own[k] if leaving is None else leaving + from_own[k]
        back_x, back_y, _ = lattice_dirs[back[k]]
        for sign, value in ((x, from_halo[k]), (back_x, from_own[k])):
            if sign != 0:
                flow_x = flow_x + value if sign > 0 else flow_x - value
        for sign, value in ((y, from_halo[k]), (back_y, from_own[k])):
            if sign != 0:
                flow_y = flow_y + value if sign > 0 else flow_y - value
    inverse = 1.0 / density
    vel_x = flow_x * inverse
    vel_y = flow_y * inverse
    towards = (arriving - leaving) * inverse
    usq = vel_x * vel_x + vel_y * vel_y + towards * towards
    keep = 1.0 - relax
    gain = relax * density
    base = gain - (1.5 * gain) * usq
    scaled = {w: (w * base, (3.0 * w) * gain, (4.5 * w) * gain) for w in lattice_weights[1::6]}
    result = []
    for k in range(5):
        x, y, _ = lattice_dirs[ways[k]]
        along = towards
        if x != 0:
            along = along + vel_x if x > 0 else along - vel_x
        if y != 0:
            along = along + vel_y if y > 0 else along - vel_y
        still, linear, square = scaled[lattice_weights[ways[k]]]
        equil = still + (linear + square * along) * along
        result.append(rolled(keep * from_halo[k] + equil, y))
    return result


everything = set(range(19))


def first_kernel(f_hbm_ref, relax_hbm_ref,
                 low_ref, high_ref, relax_ref, post_ref, up_ref, down_ref,
                 f_ref, pad_ref, sems):
    odd = parity()
    copies = [pltpu.make_async_copy(relax_hbm_ref, relax_ref, sems.at[4])]
    quarters = [(plane, half) for plane in range(2) for half in range(2)]
    for n, (plane, half) in enumerate(quarters):
        part = (slice(None), plane, pl.ds(32 * half, 32), slice(None))
        copies.append(pltpu.make_async_copy(f_hbm_ref.at[part], f_ref.at[part], sems.at[n]))
    for copy in copies:
        copy.start()
    copies[0].wait()
    for n, (actual_plane, half) in enumerate(quarters):
        copies[1 + n].wait()
        plane = jnp.where(odd == 1, 1 - actual_plane, actual_plane)
        for b in range(4 * half, 4 * half + 4):
            f = {i: f_ref[actual(i, odd), actual_plane, rows_of(b), :] for i in range(19)}
            post = collided(f, relax_ref[actual_plane, rows_of(b), :], everything)
            for i in range(19):
                post_ref[i, plane, rows_of(b), :] = post[i]
                if lattice_dirs[i][0] != 0:
                    pad_ref[i, plane, pl.ds(8 + 8 * b, 8), :] = post[i]
    head = lax.broadcasted_iota(i32, (8, 128), 0) < 4
    for i in range(20):
        ends = [
            [
                (f_ref[i, plane, rows_of(b), :] if i < 19 else relax_ref[plane, rows_of(b), :])
                for plane in range(2)
            ]
            for b in (0, 7)
        ]
        low_ref[i] = jnp.where(head, ends[0][0], pltpu.roll(ends[0][1], 4, 0))
        high_ref[i] = jnp.where(head, pltpu.roll(ends[1][0], 4, 0), ends[1][1])
    for plane in range(2):
        actual_plane = jnp.where(odd == 1, 1 - plane, plane)
        out_ref, ways = (up_ref, rising) if plane == 1 else (down_ref, falling)
        for b in range(8):

            def read(i, source):
                shift = lattice_dirs[i][0]
                if shift == 0:
                    return post_ref[i, source, rows_of(b), :]
                return pad_ref[i, source, pl.ds(8 + 8 * b - shift, 8), :]

            outgoing_planes(
                storing(out_ref, b), read, plane, 1 - plane, ways,
                relax_ref[actual_plane, rows_of(b), :],
            )


def edge_kernel(low_ref, high_ref, post_ref, seam_ref, up_ref, down_ref, relax_ref):
    odd = parity()
    row_id = lax.broadcasted_iota(i32, (8, 128), 0)
    mixed_relax = []
    for plane in range(2):
        actual_plane = jnp.where(odd == 1, 1 - plane, plane)
        upper = jnp.broadcast_to(actual_plane, (8, 128)) == 1
        mixed = []
        for i in range(20):
            j = actual(i, odd) if i < 19 else i
            high = high_ref[j]
            low = low_ref[j]
            high = jnp.where(upper, pltpu.roll(high, 4, 0), high)
            low = jnp.where(upper, low, pltpu.roll(low, 4, 0))
            mixed.append(jnp.where(row_id < 4, high, low))
        post = collided(dict(enumerate(mixed[:19])), mixed[19], everything)
        relax_ref[plane] = mixed[19]
        mixed_relax.append(mixed[19])
        for i in range(19):
            seam_ref[2 * i + plane, 0:8, :] = post_ref[i, plane, 56:64, :]
            seam_ref[2 * i + plane, 8:16, :] = post[i]
            seam_ref[2 * i + plane, 16:24, :] = post_ref[i, plane, 0:8, :]

    def read(i, source):
        shift = lattice_dirs[i][0]
        at = [seam_ref[2 * i + source, pl.ds(start - shift, 8), :] for start in (4, 8, 12)]
        return jnp.where(row_id == 3, at[0], jnp.where(row_id == 4, at[2], at[1]))

    outgoing_planes(storing(up_ref, 0), read, 1, 0, rising, mixed_relax[1])
    outgoing_planes(storing(down_ref, 0), read, 0, 1, falling, mixed_relax[0])


def two_steps(own, below, above, relax, second_ref, from_below_ref, from_above_ref):
    for b in range(9):
        for plane in range(2):
            f = {}
            for i, c in enumerate(lattice_dirs):
                source = plane - c[2]
                if source in (0, 1):
                    f[i] = own(i, source, b, c[0])
                elif source < 0:
                    f[i] = below(rising.index(i), b)
                else:
                    f[i] = above(falling.index(i), b)
            post = collided(f, relax(plane, b), everything)
            for i, value in post.items():
                put(second_ref, (i, plane), b, value)
        for side, ways, back, source, plane, out_ref in (
            (below, rising, falling, 0, -1, from_below_ref),
            (above, falling, rising, 1, 2, from_above_ref),
        ):
            post = halo_collided(
                [side(5 + k, b) for k in range(5)],
                [own(i, source, b, lattice_dirs[i][0]) for i in back],
                [side(10 + n, b) for n in range(3)],
                relax(plane, b), ways, back,
            )
            for k in range(5):
                put(out_ref, (k,), b, post[k])


def streamed(second_ref, from_below_ref, from_above_ref, plane, b):
    f = {}
    for i, c in enumerate(lattice_dirs):
        source = plane - c[2]
        if source == -1:
            f[i] = get(from_below_ref, (rising.index(i),), b, c[0])
        elif source == 2:
            f[i] = get(from_above_ref, (falling.index(i),), b, c[0])
        else:
            f[i] = get(second_ref, (i, source), b, c[0])
    return f


def middle_kernel(post_ref, seam_ref, below_ref, above_ref, below_edge_ref, above_edge_ref,
                  relax_ref, relax_edge_ref,
                  third_ref, up_ref, down_ref, relax_out_ref,
                  second_ref, from_below_ref, from_above_ref):
    odd = parity()
    row_id = lax.broadcasted_iota(i32, (8, 128), 0)

    def own(i, plane, b, shift):
        if b == 8:
            return seam_ref[2 * i + plane, 8 - shift : 16 - shift, :]
        if b == 0 and shift == 1:
            return seam_ref[2 * i + plane, 15:23, :]
        if b == 7 and shift == -1:
            return seam_ref[2 * i + plane, 1:9, :]
        return post_ref[i, plane, 8 * b - shift : 8 * b - shift + 8, :]

    def joined(main_ref, edge_ref):
        def read(j, b):
            if b == 8:
                return edge_ref[j]
            if b in (0, 7):
                turned = pltpu.roll(edge_ref[j], 4, 0)
                return jnp.where(row_id == b, turned, main_ref[j, rows_of(b), :])
            return main_ref[j, rows_of(b), :]

        return read

    below = joined(below_ref, below_edge_ref)
    above = joined(above_ref, above_edge_ref)
    for b in range(8):
        relax_out_ref[0, rows_of(b), :] = below_ref[SENT, rows_of(b), :]
        relax_out_ref[3, rows_of(b), :] = above_ref[SENT, rows_of(b), :]
        for plane in range(2):
            relax_out_ref[1 + plane, rows_of(b), :] = relax_ref[
                jnp.where(odd == 1, 1 - plane, plane), rows_of(b), :
            ]
    relax_out_ref[0, rows_of(8), :] = below_edge_ref[SENT]
    relax_out_ref[3, rows_of(8), :] = above_edge_ref[SENT]
    for plane in range(2):
        relax_out_ref[1 + plane, rows_of(8), :] = relax_edge_ref[plane]

    def relax(plane, b):
        return relax_out_ref[1 + plane, rows_of(b), :]

    two_steps(own, below, above, relax, second_ref, from_below_ref, from_above_ref)
    for b in range(9):
        for plane in range(2):
            f = streamed(second_ref, from_below_ref, from_above_ref, plane, b)
            post = collided(f, relax(plane, b), everything)
            for i in range(19):
                put(third_ref, (i, plane), b, post[i])
    for b in range(9):

        def read(i, source):
            return get(third_ref, (i, source), b, lattice_dirs[i][0])

        for out_ref, near, ways in ((up_ref, 1, rising), (down_ref, 0, falling)):
            ends = {}

            def store(j, value):
                if b < 8:
                    out_ref[8 * j + b] = value
                else:
                    ends[j] = pltpu.roll(value, 2 * (j % 4) + 1, 0)

            outgoing_planes(store, read, near, 1 - near, ways, None)
            for group in range(4 if ends else 0):
                block = ends[4 * group]
                for m in range(1, min(4, SENT - 4 * group)):
                    block = jnp.where((row_id >> 1) == m, ends[4 * group + m], block)
                out_ref[8 * SENT + group] = block


def last_kernel(post_ref, below_ref, above_ref, relax_ref, inv_ref,
                f_ref, out_ref,
                second_ref, from_below_ref, from_above_ref, flow_ref):
    odd = parity()

    def side(ref):
        def read(j, b):
            if b < 8:
                return ref[8 * j + b]
            return pltpu.roll(ref[8 * SENT + j // 4], 7 - 2 * (j % 4), 0)

        return read

    below = side(below_ref)
    above = side(above_ref)

    def own(i, plane, b, shift):
        return get(post_ref, (i, plane), b, shift)

    def relax(plane, b):
        return relax_ref[1 + plane, rows_of(b), :]

    two_steps(own, below, above, relax, second_ref, from_below_ref, from_above_ref)
    upward = jnp.where(odd == 1, -velocity_scale / 128.0, velocity_scale / 128.0)
    for plane in range(2):
        actual_plane = jnp.where(odd == 1, 1 - plane, plane)
        for b in range(8):
            f = streamed(second_ref, from_below_ref, from_above_ref, plane, b)
            for i in range(19):
                f_ref[actual(i, odd), actual_plane, rows_of(b), :] = f[i]
            density, flow = moments_of(f)
            inverse = 1.0 / density
            where = pl.ds(pl.multiple_of(actual_plane * 64 + 8 * b, 8), 8)
            flow_ref[0, where, :] = flow[0] * inverse * (velocity_scale / 128.0)
            flow_ref[1, where, :] = flow[1] * inverse * (velocity_scale / 128.0)
            flow_ref[2, where, :] = flow[2] * inverse * upward
            flow_ref[3, where, :] = density * (1.0 / 128.0)
    means = [jnp.sum(flow_ref[c].T, axis=0, keepdims=True) for c in range(4)]
    packed = jnp.concatenate(means * 4, axis=0)
    inv16 = jnp.concatenate(
        [jnp.broadcast_to(inv_ref[r : r + 1, :], (4, 128)) for r in range(4)], axis=0
    )
    picked = jnp.where(inv16 >= 0, lanes(packed, jnp.maximum(inv16, 0)), 0.0)
    out_ref[...] = jnp.concatenate([picked, jnp.zeros((112, 128), f32)], axis=0).T


def lanes(table, index):
    return jnp.take_along_axis(table, index, axis=1, mode="promise_in_bounds")


def spread(block, index, rows=8):
    return jnp.broadcast_to(block[index : index + 1, :], (rows, 128))


def lookup(tables, index):
    low = index & 127
    found = [[lanes(chunk, low) for chunk in table] for table in tables]
    for mask in (128, 256, 512):
        bit = (index & mask) != 0
        found = [
            [jnp.where(bit, f[2 * j + 1], f[2 * j]) for j in range(len(f) // 2)] for f in found
        ]
    return [f[0] for f in found]


first_chunk = [0, 0, 0, 0, 0, 0, 0, 0, 0, 0, 0, 0, 0, 0, 0, 0, 0, 0, 0, 0, 0, 0, 0, 0, 0, 0, 0, 1, 1, 1, 1, 1, 1, 1, 1, 1, 1, 1, 1, 2, 2, 2, 2, 2, 2, 2, 2, 2, 3, 3, 3, 3, 3, 3, 3, 4, 4, 4, 4, 4, 5, 5, 5, 5]
last_chunk = [2, 2, 2, 2, 3, 3, 3, 3, 3, 4, 4, 4, 4, 4, 4, 4, 5, 5, 5, 5, 5, 5, 5, 5, 5, 6, 6, 6, 6, 6, 6, 6, 6, 6, 6, 6, 6, 7, 7, 7, 7, 7, 7, 7, 7, 7, 7, 7, 7, 7, 7, 7, 7, 7, 7, 7, 7, 7, 7, 7, 7, 7, 7, 7]


def sorted_entries(values):
    values = list(values)
    count = len(values)
    p = 1
    while p < count:
        k = p
        while k >= 1:
            for j in range(k % p, count - k, 2 * k):
                for i in range(min(k, count - j - k)):
                    a, b = i + j, i + j + k
                    if a // (2 * p) == b // (2 * p):
                        swap = values[a] > values[b]
                        values[a], values[b] = (
                            jnp.where(swap, values[b], values[a]),
                            jnp.where(swap, values[a], values[b]),
                        )
            k //= 2
        p *= 2
    return values


def lookup_between(table, index, first, last):
    low = index & 127
    chunk = index >> 7
    value = lanes(table[first], low)
    for c in range(first + 1, last + 1):
        value = jnp.where(chunk >= c, lanes(table[c], low), value)
    return value


def chunks(block):
    return [spread(block, chunk) for chunk in range(8)]


def pull(total, near, here):
    gaps = [n - h for n, h in zip(near, here)]
    weight = jnp.exp2(
        (-0.5 / math.log(2.0)) * (gaps[0] * gaps[0] + gaps[1] * gaps[1] + gaps[2] * gaps[2])
    )
    return tuple(t + g * weight for t, g in zip(total, gaps))


def over_list(entry, start, unroll):
    return lax.fori_loop(0, 64, entry, start, unroll=unroll)


def blank():
    return tuple(jnp.zeros((8, 128), f32) for _ in range(3))


def prep_kernel(own_in_ref, slot_ref, pos_ref, vel_ref, nbr_ref,
                own_ref, inv_ref, rank_ref, hot_ref, icnt_ref, force_ref, p8_ref, v8_ref,
                list_ref, near_ref, drift_ref, uneven_ref):
    for k in range(2):
        for z in range(2):
            own_ref[k : k + 1, z * 64 : (z + 1) * 64] = own_in_ref[z, k : k + 1, :]
    own_ref[2:8, :] = jnp.zeros((6, 128), i32)
    row_id = lax.broadcasted_iota(i32, (128, 128), 0)
    lane_id = lax.broadcasted_iota(i32, (128, 128), 1)
    own = [spread(own_ref[...], k, 128) for k in range(2)]
    own_t = [o.T for o in own]
    ranks = []
    for k in range(2):
        count = jnp.zeros((128, 128), i32)
        for other in range(2):
            count = count + jnp.where((own_t[other] == own[k]) & (row_id < lane_id), 1, 0)
        ranks.append(jnp.sum(count, axis=0, keepdims=True))
    rank_ref[...] = jnp.concatenate(ranks + [jnp.zeros((6, 128), i32)], axis=0)
    rank_t = [jnp.broadcast_to(r, (128, 128)).T for r in ranks]
    rows = []
    for r in range(4):
        cell = jnp.zeros((128, 128), i32)
        for k in range(2):
            cell = cell + jnp.where((own_t[k] == lane_id) & (rank_t[k] == r), row_id + 1, 0)
        rows.append(jnp.sum(cell, axis=0, keepdims=True) - 1)
    inv_ref[...] = jnp.concatenate(rows + [jnp.zeros((4, 128), i32)], axis=0)
    slots = slot_ref[...]
    count = jnp.zeros((128, 16), f32)
    want = lax.broadcasted_iota(i32, (16, 128), 0) >> 2
    for s in range(8):
        one = spread(slots, s, 128)
        hot = jnp.where((one >> 2) == row_id, 1.0, 0.0).astype(bf16)
        hot_ref[:, s * 128 : (s + 1) * 128] = hot
        match = jnp.where((spread(slots, s, 16) & 3) == want, 1.0, 0.0).astype(bf16)
        count = count + lax.dot_general(
            hot, match, (((1,), (1,)), ((), ())), preferred_element_type=f32
        )
    icnt_ref[...] = 1.0 / jnp.maximum(count, 1.0)
    for c in range(3):
        for s in range(8):
            p8_ref[c, s : s + 1, :] = pos_ref[c : c + 1, s * 128 : (s + 1) * 128]
            v8_ref[c, s : s + 1, :] = vel_ref[c : c + 1, s * 128 : (s + 1) * 128]
    for k in range(8):
        for part in range(8):
            list_ref[8 * k : 8 * k + 8, part, :] = nbr_ref[
                8 * k : 8 * k + 8, part * 128 : (part + 1) * 128
            ]
    ordered = sorted_entries([list_ref[k] for k in range(64)])
    uneven = jnp.zeros((8, 128), f32)
    for k, entry in enumerate(ordered):
        list_ref[k] = entry
        if first_chunk[k] > 0:
            uneven = jnp.where(entry < 128 * first_chunk[k], 1.0, uneven)
        if last_chunk[k] < 7:
            uneven = jnp.where(entry >= 128 * (last_chunk[k] + 1), 1.0, uneven)
    uneven_ref[0] = jnp.max(uneven).astype(i32)
    here = [p8_ref[c] for c in range(3)]
    tables = [chunks(h) for h in here]

    def positions(k, total):
        near = lookup(tables, list_ref[k])
        for c in range(3):
            near_ref[k, c] = near[c]
        return pull(total, near, here)

    total = over_list(positions, blank(), 32)
    for c in range(3):
        force_ref[c] = total[c]
    speeds = [chunks(v8_ref[c]) for c in range(3)]

    def drifts(k, none):
        for c, speed in enumerate(lookup(speeds, list_ref[k])):
            drift_ref[k, c] = time_step * speed
        return none

    over_list(drifts, 0, 32)


def md_kernel(arr_ref, p8_ref, v8_ref, force_ref, list_ref, near_in_ref, drift_in_ref,
              slot_ref, hot_ref, icnt_ref, f_ref, uneven_ref,
              pos_out_ref, vel_out_ref, mom_ref, f_out_ref,
              near_ref, drift_ref, pos_ref, vel_ref, sems):
    saved = [
        pltpu.make_async_copy(f_ref, f_out_ref, sems.at[0]),
        pltpu.make_async_copy(pos_ref, pos_out_ref, sems.at[1]),
        pltpu.make_async_copy(vel_ref, vel_out_ref, sems.at[2]),
    ]
    saved[0].start()
    table = arr_ref[...].T
    slots = slot_ref[...]
    source = slots >> 2
    which = slots & 3
    target = []
    for c in range(4):
        value = lanes(spread(table, c), source)
        for r in range(1, 4):
            value = jnp.where(which == r, lanes(spread(table, r * 4 + c), source), value)
        target.append(value)
    drag = friction * target[3]
    pos = [p8_ref[c] for c in range(3)]
    vel = [v8_ref[c] for c in range(3)]
    here = list(pos)
    drift = [time_step * v for v in vel]
    for step in range(MD_STEPS):
        if step == 0:
            pair = [force_ref[c] for c in range(3)]
        else:
            from_near, from_drift = (
                (near_in_ref, drift_in_ref) if step == 1 else (near_ref, drift_ref)
            )
            miss = [pos[c] - (here[c] + drift[c]) for c in range(3)]
            largest = jnp.maximum(jnp.maximum(abs(miss[0]), abs(miss[1])), abs(miss[2]))
            largest = jnp.max(jnp.max(largest, axis=0, keepdims=True), axis=1, keepdims=True)
            largest = jnp.broadcast_to(jnp.maximum(largest, 1e-30), (8, 128))
            units = [largest * (1.0 / 1023.0), largest * (1.0 / 511.0)]
            rates = [1023.0 / largest, 511.0 / largest]
            pick = (0, 0, 1)
            whole_units = [
                jnp.floor(miss[c] * rates[pick[c]] + 0.5).astype(i32) for c in range(3)
            ]
            code = (
                (whole_units[0] << 21) | ((whole_units[1] & 2047) << 10) | (whole_units[2] & 1023)
            )
            for c in range(3):
                drift[c] = drift[c] + whole_units[c].astype(f32) * units[pick[c]]
                here[c] = here[c] + drift[c]
            table = chunks(code)

            def entry(k, total, word):
                words = (word >> 21, (word << 11) >> 21, (word << 22) >> 22)
                near = []
                for c in range(3):
                    move = from_drift[k, c] + words[c].astype(f32) * units[pick[c]]
                    drift_ref[k, c] = move
                    near.append(from_near[k, c] + move)
                    near_ref[k, c] = near[c]
                return pull(total, near, here)

            def even(total):
                for k in range(64):
                    word = lookup_between(table, list_ref[k], first_chunk[k], last_chunk[k])
                    total = entry(k, total, word)
                return total

            def any_list(total):
                def one(k, total):
                    return entry(k, total, lookup([table], list_ref[k])[0])

                return over_list(one, total, 8)

            pair = lax.cond(uneven_ref[0] == 0, even, any_list, blank())
        for c in range(3):
            force = pair_strength * pair[c] + drag * (target[c] - vel[c])
            vel[c] = vel[c] + time_step * force
            pos[c] = pos[c] + time_step * vel[c]
    for c in range(3):
        for s in range(8):
            pos_ref[c : c + 1, s * 128 : (s + 1) * 128] = pos[c][s : s + 1, :]
            vel_ref[c : c + 1, s * 128 : (s + 1) * 128] = vel[c][s : s + 1, :]
    saved[1].start()
    saved[2].start()
    speed = vel[0] * vel[0] + vel[1] * vel[1] + vel[2] * vel[2]
    data = vel + [speed]
    row_id = lax.broadcasted_iota(i32, (16, 128), 0)
    comp = row_id & 3
    sums = jnp.zeros((128, 16), f32)
    for s in range(8):
        value = spread(data[0], s, 16)
        for c in range(1, 4):
            value = jnp.where(comp == c, spread(data[c], s, 16), value)
        value = jnp.where((spread(slots, s, 16) & 3) == (row_id >> 2), value, 0.0)
        hot = hot_ref[:, s * 128 : (s + 1) * 128]
        for _ in range(3):
            piece = value.astype(bf16)
            value = value - piece.astype(f32)
            sums = sums + lax.dot_general(
                hot, piece, (((1,), (1,)), ((), ())), preferred_element_type=f32
            )
    mom_ref[...] = jnp.zeros((128, 128), f32)
    mom_ref[:, :16] = sums * icnt_ref[...]
    for copy in saved:
        copy.wait()


def cell_kernel(back_ref, own_ref, rank_ref, out_ref):
    table = back_ref[...].T[:16, :]
    which = lax.broadcasted_iota(i32, (16, 128), 0) >> 2
    total = jnp.zeros((16, 128), f32)
    for k in range(2):
        picked = lanes(table, spread(own_ref[...], k, 16))
        total = total + jnp.where(spread(rank_ref[...], k, 16) == which, picked, 0.0)
    cell = total[0:4] + total[4:8] + total[8:12] + total[12:16]
    out_ref[:, 0, :] = cell[:, :64]
    out_ref[:, 1, :] = cell[:, 64:]


room = pltpu.CompilerParams(vmem_limit_bytes=16 << 20)


def shape(*dims, dtype=f32):
    return jax.ShapeDtypeStruct(dims, dtype)


def exchange(rows):
    return lax.all_to_all(rows, ("slab", "md"), split_axis=0, concat_axis=0, tiled=True)


near_pairs = [(i, i ^ 1) for i in range(32)]
far_pairs = [(i, (i + 1) % 32 if i % 2 else (i - 1) % 32) for i in range(32)]


def whole(populations, relax, owners, positions, velocities, neighbours, atom_slots):
    hbm = pl.BlockSpec(memory_space=pltpu.HBM)
    vmem = pl.BlockSpec(memory_space=pltpu.VMEM)
    smem = pl.BlockSpec(memory_space=pltpu.SMEM)
    slots = atom_slots.reshape(8, 128)
    eights = shape(3, 8, 128)
    own, inv, rank, hot, icnt, force, p8, v8, lists, near, drift, uneven = pl.pallas_call(
        prep_kernel,
        out_shape=(
            shape(8, 128, dtype=i32),
            shape(8, 128, dtype=i32),
            shape(8, 128, dtype=i32),
            shape(128, 1024, dtype=bf16),
            shape(128, 16),
            eights,
            eights,
            eights,
            shape(64, 8, 128, dtype=i32),
            shape(64, 3, 8, 128),
            shape(64, 3, 8, 128),
            shape(1, dtype=i32),
        ),
        in_specs=[vmem] * 5,
        out_specs=(vmem,) * 11 + (smem,),
        name="prep", compiler_params=room,
    )(owners.transpose(0, 2, 1), slots, positions, velocities, neighbours.T)
    low, high, relax, post, up, down = pl.pallas_call(
        first_kernel,
        in_specs=[hbm, hbm],
        out_shape=(
            pltpu.VMEM((20, 8, 128), f32),
            pltpu.VMEM((20, 8, 128), f32),
            pltpu.VMEM((2, 64, 128), f32),
            pltpu.VMEM((19, 2, 64, 128), f32),
            pltpu.VMEM((SENT + 1, 64, 128), f32),
            pltpu.VMEM((SENT + 1, 64, 128), f32),
        ),
        scratch_shapes=[
            pltpu.VMEM((19, 2, 64, 128), f32),
            pltpu.VMEM((19, 2, 80, 128), f32),
            pltpu.SemaphoreType.DMA((5,)),
        ],
        name="first", compiler_params=room,
    )(
        pltpu.with_memory_space_constraint(populations, pltpu.HBM),
        pltpu.with_memory_space_constraint(relax, pltpu.HBM),
    )
    below = lax.ppermute(down, "slab", far_pairs)
    from_low = lax.ppermute(high, "md", [(i, (i + 1) % 4) for i in range(4)])
    from_high = lax.ppermute(low, "md", [((i + 1) % 4, i) for i in range(4)])
    above = lax.ppermute(up, "slab", near_pairs)
    seam, up_edge, down_edge, relax_edge = pl.pallas_call(
        edge_kernel,
        out_shape=(
            shape(38, 24, 128),
            shape(SENT + 1, 8, 128),
            shape(SENT + 1, 8, 128),
            shape(2, 8, 128),
        ),
        name="edge", compiler_params=room,
    )(from_low, from_high, post)
    below_edge = lax.ppermute(down_edge, "slab", far_pairs)
    above_edge = lax.ppermute(up_edge, "slab", near_pairs)
    scratch = [
        pltpu.VMEM((19, 2, PAD, 128), f32),
        pltpu.VMEM((5, PAD, 128), f32),
        pltpu.VMEM((5, PAD, 128), f32),
    ]
    post, up, down, relax_all = pl.pallas_call(
        middle_kernel,
        out_shape=(
            shape(19, 2, PAD, 128),
            shape(8 * SENT + 4, 8, 128),
            shape(8 * SENT + 4, 8, 128),
            shape(4, ROWS, 128),
        ),
        scratch_shapes=scratch,
        name="middle", compiler_params=room,
    )(post, seam, below, above, below_edge, above_edge, relax, relax_edge)
    below = lax.ppermute(down, "slab", far_pairs)
    above = lax.ppermute(up, "slab", near_pairs)
    f, outgoing = pl.pallas_call(
        last_kernel,
        out_shape=(pltpu.VMEM((19, 2, 64, 128), f32), shape(128, 128)),
        scratch_shapes=scratch + [pltpu.VMEM((4, 128, 128), f32)],
        name="last", compiler_params=room,
    )(post, below, above, relax_all, inv)
    arrived = exchange(outgoing)
    pos_out, vel_out, moms, f_out = pl.pallas_call(
        md_kernel,
        in_specs=[vmem] * 11 + [smem],
        out_specs=(hbm, hbm, vmem, hbm),
        out_shape=(
            shape(3, 1024), shape(3, 1024), shape(128, 128), shape(19, 2, 64, 128)
        ),
        scratch_shapes=[
            pltpu.VMEM((64, 3, 8, 128), f32),
            pltpu.VMEM((64, 3, 8, 128), f32),
            pltpu.VMEM((3, 1024), f32),
            pltpu.VMEM((3, 1024), f32),
            pltpu.SemaphoreType.DMA((3,)),
        ],
        name="md", compiler_params=room,
    )(arrived, p8, v8, force, lists, near, drift, slots, hot, icnt, f, uneven)
    returned = exchange(moms)
    cell = pl.pallas_call(
        cell_kernel, out_shape=shape(4, 2, 64), name="cells", compiler_params=room
    )(returned, own, rank)
    return (f_out, pos_out, vel_out, cell)


def solution(mesh):
    return jax.shard_map(
        whole,
        mesh=mesh,
        in_specs=(
            P(None, "slab", "md", None),
            P("slab", "md", None),
            P("slab", "md", None),
            P(None, ("slab", "md")),
            P(None, ("slab", "md")),
            P(("slab", "md"), None),
            P(("slab", "md")),
        ),
        out_specs=(
            P(None, "slab", "md", None),
            P(None, ("slab", "md")),
            P(None, ("slab", "md")),
            P(None, "slab", "md"),
        ),
        check_vma=False,
    )
```
